128 devices in a mesh: groups: 4 (over y, x), row: 32 (over z, core).
Axes of the slice: x: 2, y: 2, z: 16, core: 2. Of those that a mesh axis runs over, the one named last changes fastest.
The devices are a block of a 8x8x16 slice.
Arguments:
- design_matrix: bfloat16 [2048, 65536], P('groups', 'row'), parts along dimension 0, may hold values from -0.078125 to 0.078125
- targets: float32 [2048, 128], P(('groups', 'row')), parts along dimension 0, may hold values from -24 to 24
- linear: float32 [262144, 128], P(('groups', 'row')), parts along dimension 0, may hold values from -24 to 24
- diagonal: float32 [262144], P(('groups', 'row')), parts along dimension 0, may hold values from 0.1 to 2
- lower_code: int32 [262144, 128], P(('groups', 'row')), parts along dimension 0, may hold values from -192 to -17
- upper_code: int32 [262144, 128], P(('groups', 'row')), parts along dimension 0, may hold values from 16 to 191
Outputs:
- box_iterate: float32 [262144, 128], P(('groups', 'row')), parts along dimension 0
- scaled_dual: float32 [262144, 128], P(('groups', 'row')), parts along dimension 0
The draws below stay inside these ranges and needn't reach their ends.
There are 4 independent parts, one for each index of `groups`. The reference program is written for one: setup_inputs(seed, part) draws one part's arguments, and reference() takes and returns one part's arrays. A program takes and returns all parts, laid end to end along the dimension named above; each array names one. Nothing has to cross between parts.
All inputs are finite; a program needn't handle non-finite values.
Results may differ from the reference program's by a relative error of at most 0.00033.
Values may be sent and summed in bfloat16 or wider, within the bound.
A program may use at most 128 MiB of HBM per device.

```python
import math
import jax
import jax.numpy as jnp
from jax import lax

N = 65536
K = 512
S = 128
ITERS = 4
DEPTH = 5


def place_ends(drawn, own_key, least, largest):
    longest = drawn.shape.index(max(drawn.shape))
    spots = []
    for shift in (0, 1):
        where = [jax.random.randint(jax.random.fold_in(own_key, axis), (), 0, length) for axis, length in enumerate(drawn.shape)]
        where[longest] = (where[longest] + shift) % drawn.shape[longest]
        spots.append(tuple(where))
    return drawn.at[spots[0]].set(least).at[spots[1]].set(largest)


def raised(array, key, source, target, shards_of, factor):
    def block_of(position):
        return (jnp.arange(array.shape[position]) // (array.shape[position] // shards_of)).reshape((-1,) + (1,) * (array.ndim - 1 - position))

    near = jax.random.permutation(key, shards_of)[block_of(target)]
    far = (block_of(target) + shards_of // 2) % shards_of
    return jnp.where((block_of(source) == near) | (block_of(source) == far), factor * array, array)


def level_of(key, extent, pieces, smallest, largest):
    loudness = 1.0
    for dim, shards_of in pieces:
        draws = jax.random.uniform(jax.random.fold_in(jax.random.fold_in(key, 6), dim), (shards_of,), jnp.float32, smallest / len(pieces), largest / len(pieces))
        loudness = loudness * jnp.repeat(jnp.exp(draws), extent[dim] // shards_of).reshape((-1,) + (1,) * (len(extent) - 1 - dim))
    return loudness


def gaussian(rng, extent, deviation, bound, shards=(), kind=jnp.bfloat16):
    values = jax.random.normal(rng, extent, jnp.float32) * deviation
    if len(shards) > 0:
        values = level_of(rng, extent, shards, -0.22, 0.18) * values
    return jnp.clip(values, min=-bound, max=bound).astype(kind)


def noise_with(own_key, extent, spread, reach, shards, heavy, held_as=jnp.bfloat16):
    values = spread * jax.random.normal(own_key, extent, jnp.float32)
    if shards:
        values = values * level_of(own_key, extent, shards, -0.22, 0.18)
    return jnp.clip(raised(values, jax.random.fold_in(own_key, 3), *heavy), -reach, reach).astype(held_as)


def setup_inputs(seed: int = 0, part: int = 0) -> dict:
    key_of = jax.random.split(jax.random.key(seed), 7)
    part_keys = jax.random.split(jax.random.fold_in(key_of[6], part), 7)
    design_matrix = noise_with(part_keys[0], (K, N), (max(N // 3, 2 * K)) ** -0.5, 0.078125, ((1, 32),), (1, 0, 32, 2.75))
    targets = gaussian(part_keys[1], (K, S), 4.0, 24.0, ((0, 32),), jnp.float32)
    linear = gaussian(part_keys[2], (N, S), 4.0, 24.0, ((0, 32),), jnp.float32)
    diagonal = jnp.clip(jnp.exp(math.log(2.0) - 2.9957323 * jax.random.uniform(part_keys[3], (N,), jnp.float32) ** level_of(part_keys[3], (N,), ((0, 32),), -0.2, 0.2)), 0.1, 2.0)
    lower_code = place_ends(jax.random.randint(part_keys[4], (N, S), -192, -16), jax.random.fold_in(part_keys[4], 1), -192, (-16) - 1).astype(jnp.int32)
    upper_code = place_ends(jax.random.randint(part_keys[5], (N, S), 16, 192), jax.random.fold_in(part_keys[5], 1), 16, 191).astype(jnp.int32)
    return {"design_matrix": design_matrix, "targets": targets, "linear": linear, "diagonal": diagonal, "lower_code": lower_code, "upper_code": upper_code}


rho_plus_lip = 7.0


def solve_small(matrix, rhs):
    count = len(rhs)
    table = [list(line) for line in matrix]
    right = list(rhs)
    for p in range(count):
        for i in range(p + 1, count):
            factor = table[i][p] / table[p][p]
            for j in range(p, count):
                table[i][j] = table[i][j] - factor * table[p][j]
            right[i] = right[i] - factor * right[p]
    result = [None] * count
    for i in reversed(range(count)):
        total = right[i]
        for j in range(i + 1, count):
            total = total - table[i][j] * result[j]
        result[i] = total / table[i][i]
    return result


def mix_weights(gram):
    count = len(gram)
    trace = gram[0][0]
    for i in range(1, count):
        trace = trace + gram[i][i]
    shift = 0.01 * trace / count + 1e-6
    matrix = [[gram[i][j] + (shift if i == j else 0.0) for j in range(count)] for i in range(count)]
    solved = solve_small(matrix, [jnp.ones_like(trace)] * count)
    total = solved[0]
    for i in range(1, count):
        total = total + solved[i]
    return [item / total for item in solved]


def reference(design_matrix, targets, linear, diagonal, lower_code, upper_code):
    lower = lower_code.astype(jnp.float32) / 64.0
    upper = upper_code.astype(jnp.float32) / 64.0
    step_size = (1.0 / (rho_plus_lip + diagonal))[:, None]

    def apply_map(state):
        point = state[0] - state[1]
        point_b = point.astype(jnp.bfloat16)
        product = jnp.dot(design_matrix, point_b, preferred_element_type=jnp.float32)
        misfit = (product - targets).astype(jnp.bfloat16)
        gradient = lax.dot_general(design_matrix, misfit, (((0,), (0,)), ((), ())), preferred_element_type=jnp.float32)
        gradient = gradient + diagonal[:, None] * point + linear
        moved = point - step_size * gradient
        boxed = jnp.clip(moved + state[1], lower, upper)
        scaled = state[1] + moved - boxed
        return jnp.stack([boxed, scaled])

    state = jnp.zeros((2,) + linear.shape, jnp.float32)
    hist_mapped = []
    hist_change = []
    for iteration in range(ITERS):
        mapped = apply_map(state)
        hist_mapped.append(mapped)
        hist_change.append(mapped - state)
        if len(hist_mapped) > DEPTH:
            hist_mapped.pop(0)
            hist_change.pop(0)
        stacked = jnp.stack(hist_change)
        whole = jnp.einsum('icns,jcns->ijs', stacked, stacked, precision=lax.Precision.HIGHEST)
        count = len(hist_change)
        gram = [[whole[i, j] for j in range(count)] for i in range(count)]
        alpha = mix_weights(gram)
        combined = alpha[0][None, None, :] * hist_mapped[0]
        for i in range(1, count):
            combined = combined + alpha[i][None, None, :] * hist_mapped[i]
        state = jnp.stack([jnp.clip(combined[0], lower, upper), combined[1]])
    return state[0], state[1]
```

```python
import functools

import jax
import jax.numpy as jnp
from jax import lax
from jax.experimental import pallas as pl
from jax.experimental.pallas import tpu as pltpu
from jax.sharding import PartitionSpec as P

ITERS = 4
WINDOW = 4
CHUNK = 256
rho_plus_lip = 7.0
F32, BF16 = jnp.float32, jnp.bfloat16
SENT_A, SENT_B = jnp.bfloat16, jnp.bfloat16


def solve_small(matrix, rhs):
    count = len(rhs)
    table = [list(line) for line in matrix]
    right = list(rhs)
    for p in range(count):
        for i in range(p + 1, count):
            factor = table[i][p] / table[p][p]
            for j in range(p, count):
                table[i][j] = table[i][j] - factor * table[p][j]
            right[i] = right[i] - factor * right[p]
    result = [None] * count
    for i in reversed(range(count)):
        total = right[i]
        for j in range(i + 1, count):
            total = total - table[i][j] * result[j]
        result[i] = total / table[i][i]
    return result


def mix_weights(gram):
    count = len(gram)
    trace = gram[0][0]
    for i in range(1, count):
        trace = trace + gram[i][i]
    shift = 0.01 * trace / count + 1e-06
    matrix = [[gram[i][j] + (shift if i == j else 0.0) for j in range(count)] for i in range(count)]
    solved = solve_small(matrix, [jnp.ones_like(trace)] * count)
    total = solved[0]
    for i in range(1, count):
        total = total + solved[i]
    return [item / total for item in solved]


def folded(value):
    return jnp.sum(value.reshape(-1, 8, value.shape[-1]), axis=0)


def kernel(
    devices,
    a_hbm, targets_hbm, linear_hbm, diagonal_hbm, lower_hbm, upper_hbm,
    z_hbm, u_hbm,
    a, a_t, linear, diagonal, code, low, high, dd, ss,
    mz, mu, cz, cu, sz, su, xb, pf, pb, known_a, ra, wb, known_b, window, m, targets, gp, ga, gw,
    load_sem, out_sem, send_sem, recv_sem,
):
    chips = devices // 2
    quarters = chips // WINDOW
    rows, n = a.shape
    block = rows // (2 * WINDOW)
    piece = block // quarters
    s = linear.shape[1]
    me = lax.axis_index("row")
    chip, core = me // 2, me % 2
    spot, quarter = chip % WINDOW, chip // WINDOW
    own = pl.multiple_of((2 * spot + core) * block, block)
    toward = 2 - 4 * core

    def at(offset, which):
        return 2 * ((chip + offset + chips) % chips) + which

    def owned_by(offset, which):
        return pl.multiple_of((2 * ((chip + offset + chips) % WINDOW) + which) * block, block)

    owners = [(at(0, 1 - core), owned_by(0, 1 - core), 0)]
    served = [at(0, 1 - core)]
    for offset, slot in ((1, 1), (-1, 3)):
        for which in (0, 1):
            owners.append((at(offset, which), owned_by(offset, which), slot + core))
            served.append(at(offset, which))
    for which in (0, 1):
        owners.append((at(toward, which), owned_by(toward, which), 5 + core))
    served += [at(-2, 0), at(2, 1)]
    sharers = [at(WINDOW * i, core) for i in range(1, quarters)]

    def send(source, target, device, index, arrival):
        copy = pltpu.make_async_remote_copy(
            src_ref=source,
            dst_ref=target,
            send_sem=send_sem.at[index],
            recv_sem=recv_sem.at[arrival],
            device_id={"row": device},
            device_id_type=pl.DeviceIdType.MESH,
        )
        copy.start()
        return copy

    def arrived(buffer, arrival):
        pltpu.make_async_remote_copy(
            src_ref=buffer,
            dst_ref=buffer,
            send_sem=send_sem.at[0],
            recv_sem=recv_sem.at[arrival],
            device_id={"row": at(0, 1 - core)},
            device_id_type=pl.DeviceIdType.MESH,
        ).wait_recv()

    def sent(copies):
        for copy in copies:
            copy.wait_send()

    def load(source, target, index):
        copy = pltpu.make_async_copy(source, target, load_sem.at[index])
        copy.start()
        return copy

    share = pl.ds(pl.multiple_of(quarter * piece, piece), piece)
    load_targets = load(targets_hbm, targets.at[share], 0)

    def load_a(i, carry):
        place, part = i // quarters, i % quarters
        source = pl.multiple_of((part * 2 * WINDOW + place) * piece, piece)
        target = pl.multiple_of(i * piece, piece)
        pltpu.make_async_copy(
            a_hbm.at[pl.ds(source, piece)], a.at[pl.ds(target, piece)], load_sem.at[1]
        ).start()
        return carry

    lax.fori_loop(0, 2 * WINDOW * quarters, load_a, 0)
    loads = [
        load(diagonal_hbm, diagonal, 2),
        load(lower_hbm, code.at[0], 3),
        load(upper_hbm, code.at[1], 4),
        load(linear_hbm, linear, 5),
    ]

    barrier = pltpu.get_barrier_semaphore()
    near = [at(0, 1 - core), at(1, 0), at(1, 1), at(-1, 0), at(-1, 1)]
    near += [at(toward, 0), at(toward, 1), at(-toward, core)]
    greeted = sharers + near
    for device in greeted:
        pl.semaphore_signal(
            barrier, inc=1, device_id={"row": device}, device_id_type=pl.DeviceIdType.MESH
        )

    load_targets.wait()
    pltpu.make_async_copy(a_hbm, a, load_sem.at[1]).wait()
    for copy in loads:
        copy.wait()

    def prepare(i, carry):
        part = pl.ds(pl.multiple_of(i * 128, 128), 128)
        a_t[part, :] = jnp.transpose(a[:, part])
        d = jnp.transpose(jnp.broadcast_to(diagonal[pl.ds(i, 1), :], (128, 128)))
        dd[part, :] = d
        ss[part, :] = 1.0 / (rho_plus_lip + d)
        low[part, :] = code[0, part, :].astype(F32) * (1.0 / 64.0)
        high[part, :] = code[1, part, :].astype(F32) * (1.0 / 64.0)
        return carry

    lax.fori_loop(0, n // 128, prepare, 0)
    pl.semaphore_wait(barrier, len(greeted))

    copies = [
        send(targets.at[share], targets.at[share], device, i, 0)
        for i, device in enumerate(sharers)
    ]
    arrived(targets.at[pl.ds(0, (quarters - 1) * piece)], 0)
    sent(copies)

    gram = []
    first = None
    for it in range(ITERS):
        mine = pl.ds(own, block)
        if it == 0:
            m[mine, :] = (0.0 - targets[...]).astype(BF16)
        else:
            def multiplied(i, carry):
                part = pl.ds(pl.multiple_of(i * 128, 128), 128)
                product = jnp.dot(a[part, :], xb[...], preferred_element_type=F32)
                pf[part, :] = product
                if it == 1:
                    rounded = product.astype(SENT_A)
                    known_a[part, :] = rounded.astype(F32)
                else:
                    known = known_a[part, :]
                    rounded = (product - known).astype(SENT_A)
                    known_a[part, :] = known + rounded.astype(F32)
                pb[part, :] = rounded
                return carry

            lax.fori_loop(0, rows // 128, multiplied, 0)
            copies = [
                send(pb.at[pl.ds(start, block)], ra.at[slot], device, i, 1)
                for i, (device, start, slot) in enumerate(owners)
            ]
            arrived(ra, 1)
            total = ra[0].astype(F32)
            for i in range(1, len(owners)):
                total = total + ra[i].astype(F32)
            if it > 1:
                total = total + window[...]
            window[...] = total
            total = total + pf[mine, :]
            if it > 1:
                total = total - known_b[0]
            rounded = total.astype(SENT_B)
            wb[quarter] = rounded
            known_b[0] = rounded.astype(F32) + (known_b[0] if it > 1 else 0.0)
            sent(copies)
            copies = [
                send(wb.at[quarter], wb.at[quarter], device, i, 2)
                for i, device in enumerate(sharers)
            ]
            arrived(wb.at[pl.ds(0, quarters - 1)], 2)
            sent(copies)
            total = wb[0].astype(F32)
            for i in range(1, quarters):
                total = total + wb[i].astype(F32)
            if it > 1:
                total = total + known_b[1]
            known_b[1] = total
            m[mine, :] = (total - targets[...]).astype(BF16)
        copies = [send(m.at[mine], m.at[mine], device, i, 3) for i, device in enumerate(served)]
        arrived(m.at[pl.ds(0, rows - block)], 3)
        sent(copies)

        def mapped(i, sums):
            part = pl.ds(pl.multiple_of(i * CHUNK, CHUNK), CHUNK)
            gradient = jnp.dot(a_t[part, :], m[...], preferred_element_type=F32)
            if it == 0:
                value = -ss[part, :] * (gradient + linear[part, :])
                z = jnp.minimum(jnp.maximum(value, low[part, :]), high[part, :])
                u = value - z
                mz[0, part, :] = z
                mu[0, part, :] = u
                xb[part, :] = (z - u).astype(BF16)
                return (sums[0] + folded(z * z + u * u),)
            z0, u0 = (mz[0, part, :], mu[0, part, :]) if it == 1 else (sz[part, :], su[part, :])
            point = z0 - u0
            gradient = gradient + dd[part, :] * point + linear[part, :]
            value = u0 + (point - ss[part, :] * gradient)
            z = jnp.minimum(jnp.maximum(value, low[part, :]), high[part, :])
            u = value - z
            mz[it, part, :] = z
            mu[it, part, :] = u
            dz, du = z - z0, u - u0
            if it < ITERS - 1:
                cz[it - 1, part, :] = dz
                cu[it - 1, part, :] = du
            out = []
            for j in range(it):
                pz, pu = (
                    (mz[0, part, :], mu[0, part, :])
                    if j == 0
                    else (cz[j - 1, part, :], cu[j - 1, part, :])
                )
                out.append(sums[j] + folded(pz * dz + pu * du))
            out.append(sums[it] + folded(dz * dz + du * du))
            return tuple(out)

        zero = jnp.zeros((8, s), F32)
        sums = lax.fori_loop(0, n // CHUNK, mapped, (zero,) * (it + 1))
        sums = [jnp.sum(item, axis=0, keepdims=True) for item in sums]
        if it == 0:
            first = sums[0]
            continue
        shared = ([first] if it == 1 else []) + sums
        for i in range(4):
            gp[pl.ds(i, 1), :] = shared[i] if i < len(shared) else jnp.zeros((1, s), F32)
        copies = [
            send(gp, ga.at[slot], device, i, 4) for i, (device, _, slot) in enumerate(owners)
        ]
        total = gp[...]
        arrived(ga, 4)
        for i in range(len(owners)):
            total = total + ga[i]
        gw[quarter] = total
        sent(copies)
        copies = [
            send(gw.at[quarter], gw.at[quarter], device, i, 5) for i, device in enumerate(sharers)
        ]
        arrived(gw.at[pl.ds(0, quarters - 1)], 5)
        sent(copies)
        total = gw[0]
        for i in range(1, quarters):
            total = total + gw[i]
        lines = [total[i : i + 1, :] for i in range(len(shared))]
        if it == 1:
            gram = [[lines[0]]]
            lines = lines[1:]
        for i in range(it):
            gram[i].append(lines[i])
        gram.append(lines)
        alpha = mix_weights(gram)

        def combined(i, carry):
            part = pl.ds(pl.multiple_of(i * CHUNK, CHUNK), CHUNK)
            z = alpha[0] * mz[0, part, :]
            u = alpha[0] * mu[0, part, :]
            for j in range(1, it + 1):
                z = z + alpha[j] * mz[j, part, :]
                u = u + alpha[j] * mu[j, part, :]
            z = jnp.minimum(jnp.maximum(z, low[part, :]), high[part, :])
            sz[part, :] = z
            su[part, :] = u
            if it < ITERS - 1:
                xb[part, :] = (z - u).astype(BF16)
            else:
                pltpu.make_async_copy(sz.at[part], z_hbm.at[part], out_sem.at[0]).start()
                pltpu.make_async_copy(su.at[part], u_hbm.at[part], out_sem.at[1]).start()
            return carry

        lax.fori_loop(0, n // CHUNK, combined, 0)
    pltpu.make_async_copy(sz, z_hbm, out_sem.at[0]).wait()
    pltpu.make_async_copy(su, u_hbm, out_sem.at[1]).wait()


def per_device(devices, design_matrix, targets, linear, diagonal, lower_code, upper_code):
    rows, n = design_matrix.shape
    s = linear.shape[1]
    quarters = devices // 2 // WINDOW
    block = rows // (2 * WINDOW)
    others = 2 * WINDOW - 1
    full = pltpu.VMEM((n, s), F32)
    hbm = pl.BlockSpec(memory_space=pl.ANY)
    return pl.pallas_call(
        functools.partial(kernel, devices),
        out_shape=(jax.ShapeDtypeStruct((n, s), F32),) * 2,
        in_specs=[hbm] * 6,
        out_specs=(hbm, hbm),
        scratch_shapes=[
            pltpu.VMEM((rows, n), BF16),
            pltpu.VMEM((n, rows), BF16),
            full,
            pltpu.VMEM((n // 128, 128), F32),
            pltpu.VMEM((2, n, s), jnp.int32),
            full,
            full,
            full,
            full,
            pltpu.VMEM((ITERS, n, s), F32),
            pltpu.VMEM((ITERS, n, s), F32),
            pltpu.VMEM((ITERS - 2, n, s), F32),
            pltpu.VMEM((ITERS - 2, n, s), F32),
            full,
            full,
            pltpu.VMEM((n, s), BF16),
            pltpu.VMEM((rows, s), F32),
            pltpu.VMEM((rows, s), SENT_A),
            pltpu.VMEM((rows, s), F32),
            pltpu.VMEM((others, block, s), SENT_A),
            pltpu.VMEM((quarters, block, s), SENT_B),
            pltpu.VMEM((2, block, s), F32),
            pltpu.VMEM((block, s), F32),
            pltpu.VMEM((rows, s), BF16),
            pltpu.VMEM((block, s), F32),
            pltpu.VMEM((4, s), F32),
            pltpu.VMEM((others, 4, s), F32),
            pltpu.VMEM((quarters, 4, s), F32),
            pltpu.SemaphoreType.DMA((6,)),
            pltpu.SemaphoreType.DMA((2,)),
            pltpu.SemaphoreType.DMA((others,)),
            pltpu.SemaphoreType.DMA((6,)),
        ],
        compiler_params=pltpu.CompilerParams(
            collective_id=0, has_side_effects=True, vmem_limit_bytes=56 * 1024 * 1024
        ),
        name="admm",
    )(
        design_matrix,
        targets,
        linear,
        diagonal.reshape(n // 128, 128),
        lower_code,
        upper_code,
    )


def solution(mesh):
    in_specs = (
        P("groups", "row"),
        P(("groups", "row"), None),
        P(("groups", "row"), None),
        P(("groups", "row")),
        P(("groups", "row"), None),
        P(("groups", "row"), None),
    )
    out_specs = (P(("groups", "row"), None), P(("groups", "row"), None))
    return jax.shard_map(
        functools.partial(per_device, mesh.shape["row"]),
        mesh=mesh,
        in_specs=in_specs,
        out_specs=out_specs,
        check_vma=False,
    )
```

```python
import functools

import jax
import jax.numpy as jnp
from jax import lax
from jax.experimental import pallas as pl
from jax.experimental.pallas import tpu as pltpu
from jax.sharding import PartitionSpec as P

ITERS = 4
WINDOW = 4
CHUNK = 256
rho_plus_lip = 7.0
F32, BF16 = jnp.float32, jnp.bfloat16
SENT_A, SENT_B = jnp.bfloat16, jnp.bfloat16


def solve_small(matrix, rhs):
    count = len(rhs)
    table = [list(line) for line in matrix]
    right = list(rhs)
    inverse = []
    for p in range(count):
        inverse.append(1.0 / table[p][p])
        for i in range(p + 1, count):
            factor = table[i][p] * inverse[p]
            for j in range(p + 1, count):
                table[i][j] = table[i][j] - factor * table[p][j]
            right[i] = right[i] - factor * right[p]
    result = [None] * count
    for i in reversed(range(count)):
        total = right[i]
        for j in range(i + 1, count):
            total = total - table[i][j] * result[j]
        result[i] = total * inverse[i]
    return result


def mix_weights(gram):
    count = len(gram)
    trace = gram[0][0]
    for i in range(1, count):
        trace = trace + gram[i][i]
    shift = 0.01 * trace / count + 1e-06
    matrix = [[gram[i][j] + (shift if i == j else 0.0) for j in range(count)] for i in range(count)]
    solved = solve_small(matrix, [jnp.ones_like(trace)] * count)
    total = solved[0]
    for i in range(1, count):
        total = total + solved[i]
    inverse = 1.0 / total
    return [item * inverse for item in solved]


def folded(value):
    return jnp.sum(value.reshape(-1, 8, value.shape[-1]), axis=0)


def kernel(
    devices,
    a_hbm, targets_hbm, linear_hbm, diagonal_hbm, lower_hbm, upper_hbm,
    z_hbm, u_hbm,
    a, a_t, linear, diagonal, code, low, high, dd, ss,
    mz, mu, cz, cu, sz, su, base, xb, pf, pb, known_a, ra, wb, known_b, window, m, targets, ga_1, ga_2, ga_3,
    load_sem, out_sem, send_sem, recv_sem,
):
    chips = devices // 2
    quarters = chips // WINDOW
    rows, n = a.shape
    block = rows // (2 * WINDOW)
    piece = block // quarters
    s = linear.shape[1]
    me = lax.axis_index("row")
    chip, core = me // 2, me % 2
    spot, quarter = chip % WINDOW, chip // WINDOW
    own = pl.multiple_of((2 * spot + core) * block, block)
    toward = 2 - 4 * core

    def at(offset, which):
        return 2 * ((chip + offset + chips) % chips) + which

    def owned_by(offset, which):
        return pl.multiple_of((2 * ((chip + offset + chips) % WINDOW) + which) * block, block)

    served = [at(-2, 0), at(2, 1)]
    for offset in (1, -1):
        for which in (0, 1):
            served.append(at(offset, which))
    served.append(at(0, 1 - core))
    def everyone(source, target, arrival):
        def chips_away(i, carry):
            away = (chips // 2 - (i + 1) // 2) * (1 - 2 * ((i + 1) % 2))
            for which in (0, 1):
                send(source, target, at(away, which), arrival, arrival)
            return carry

        lax.fori_loop(0, chips - 1, chips_away, 0)
        send(source, target, at(0, 1 - core), arrival, arrival)

    def left(buffer, index):
        pltpu.make_async_remote_copy(
            src_ref=buffer,
            dst_ref=buffer,
            send_sem=send_sem.at[index],
            recv_sem=recv_sem.at[0],
            device_id={"row": at(0, 1 - core)},
            device_id_type=pl.DeviceIdType.MESH,
        ).wait_send()

    sharers = [at(WINDOW * i, core) for i in range(1, quarters)]

    def send(source, target, device, index, arrival):
        copy = pltpu.make_async_remote_copy(
            src_ref=source,
            dst_ref=target,
            send_sem=send_sem.at[index],
            recv_sem=recv_sem.at[arrival],
            device_id={"row": device},
            device_id_type=pl.DeviceIdType.MESH,
        )
        copy.start()
        return copy

    def arrived(buffer, arrival):
        pltpu.make_async_remote_copy(
            src_ref=buffer,
            dst_ref=buffer,
            send_sem=send_sem.at[0],
            recv_sem=recv_sem.at[arrival],
            device_id={"row": at(0, 1 - core)},
            device_id_type=pl.DeviceIdType.MESH,
        ).wait_recv()

    def load(source, target, index):
        copy = pltpu.make_async_copy(source, target, load_sem.at[index])
        copy.start()
        return copy

    barrier = pltpu.get_barrier_semaphore()

    def greet(i, carry):
        away = (devices // 2 - (i + 1) // 2) * (1 - 2 * ((i + 1) % 2))
        pl.semaphore_signal(
            barrier,
            inc=1,
            device_id={"row": (me + away + devices) % devices},
            device_id_type=pl.DeviceIdType.MESH,
        )
        return carry

    lax.fori_loop(0, devices - 1, greet, 0)

    share = pl.ds(pl.multiple_of(quarter * piece, piece), piece)
    load_targets = load(targets_hbm, targets.at[share], 0)

    def load_a(i, carry):
        place, part = i // quarters, i % quarters
        source = pl.multiple_of((part * 2 * WINDOW + place) * piece, piece)
        target = pl.multiple_of(i * piece, piece)
        pltpu.make_async_copy(
            a_hbm.at[pl.ds(source, piece)], a.at[pl.ds(target, piece)], load_sem.at[1]
        ).start()
        return carry

    lax.fori_loop(0, 2 * WINDOW * quarters, load_a, 0)
    loads = [
        load(diagonal_hbm, diagonal, 2),
        load(lower_hbm, code.at[0], 3),
        load(upper_hbm, code.at[1], 4),
        load(linear_hbm, linear, 5),
    ]

    shown = pl.ds(pl.multiple_of(own + quarter * piece, piece), piece)
    load_targets.wait()
    m[shown, :] = (0.0 - targets[share, :]).astype(BF16)
    pl.semaphore_wait(barrier, devices - 1)
    everyone(m.at[shown], m.at[shown], 3)
    for device in sharers:
        send(targets.at[share], targets.at[share], device, 0, 0)

    pltpu.make_async_copy(a_hbm, a, load_sem.at[1]).wait()
    for copy in loads:
        copy.wait()

    def prepare(i, carry):
        part = pl.ds(pl.multiple_of(i * 128, 128), 128)
        a_t[part, :] = jnp.transpose(a[:, part])
        d = jnp.transpose(jnp.broadcast_to(diagonal[pl.ds(i, 1), :], (128, 128)))
        dd[part, :] = d
        ss[part, :] = 1.0 / (rho_plus_lip + d)
        low[part, :] = code[0, part, :].astype(F32) * (1.0 / 64.0)
        high[part, :] = code[1, part, :].astype(F32) * (1.0 / 64.0)
        return carry

    lax.fori_loop(0, n // 128, prepare, 0)

    arrived(m.at[pl.ds(0, rows - piece)], 3)
    left(m.at[pl.ds(0, rows - piece)], 3)

    gas = [ga_1, ga_2, ga_3]
    gram = []
    first = None
    for it in range(ITERS):
        mine = pl.ds(own, block)
        if it > 0:
            def multiplied(i, carry):
                offset = jnp.where(i == 0, toward, jnp.where(i == 3, 0, 3 - 2 * i))
                part = pl.ds(pl.multiple_of(owned_by(offset, 0), 2 * block), 2 * block)
                product = jnp.dot(a[part, :], xb[...], preferred_element_type=F32)
                pf[part, :] = product
                if it == 1:
                    rounded = product.astype(SENT_A)
                    known_a[part, :] = rounded.astype(F32)
                else:
                    known = known_a[part, :]
                    rounded = (product - known).astype(SENT_A)
                    known_a[part, :] = known + rounded.astype(F32)
                pb[part, :] = rounded

                @pl.when(i < WINDOW - 1)
                def _():
                    for which in (0, 1):
                        send(
                            pb.at[pl.ds(owned_by(offset, which), block)],
                            ra.at[2 * ((i + 2) % 3) + 1 + core],
                            at(offset, which),
                            1,
                            1,
                        )

                return carry

            def based(i, carry):
                part = pl.ds(pl.multiple_of(i * CHUNK, CHUNK), CHUNK)
                z0, u0 = (mz[0, part, :], mu[0, part, :]) if it == 1 else (sz[part, :], su[part, :])
                point = z0 - u0
                base[part, :] = z0 - ss[part, :] * (dd[part, :] * point + linear[part, :])
                return carry

            lax.fori_loop(0, WINDOW, multiplied, 0)
            send(pb.at[pl.ds(owned_by(0, 1 - core), block)], ra.at[0], at(0, 1 - core), 1, 1)
            lax.fori_loop(0, n // CHUNK, based, 0)
            arrived(ra, 1)
            total = ra[0].astype(F32)
            for i in range(1, len(served)):
                total = total + ra[i].astype(F32)
            if it > 1:
                total = total + window[...]
            window[...] = total
            total = total + pf[mine, :]
            if it > 1:
                total = total - known_b[0]
            rounded = total.astype(SENT_B)
            wb[quarter] = rounded
            known_b[0] = rounded.astype(F32) + (known_b[0] if it > 1 else 0.0)
            for device in sharers:
                send(wb.at[quarter], wb.at[quarter], device, 2, 2)
            left(ra, 1)
            arrived(wb.at[pl.ds(0, quarters - 1)], 2)
            total = wb[0].astype(F32)
            for i in range(1, quarters):
                total = total + wb[i].astype(F32)
            if it > 1:
                total = total + known_b[1]
            known_b[1] = total
            if it == 1:
                arrived(targets.at[pl.ds(0, (quarters - 1) * piece)], 0)
                left(targets.at[pl.ds(0, (quarters - 1) * piece)], 0)
            m[mine, :] = (total - targets[...]).astype(BF16)
            for device in served:
                send(m.at[mine], m.at[mine], device, 3, 3)
            left(wb.at[pl.ds(0, quarters - 1)], 2)
            arrived(m.at[pl.ds(0, rows - block)], 3)
            left(m.at[pl.ds(0, rows - block)], 3)

        def mapped(i, sums):
            part = pl.ds(pl.multiple_of(i * CHUNK, CHUNK), CHUNK)
            gradient = jnp.dot(a_t[part, :], m[...], preferred_element_type=F32)
            if it == 0:
                value = -ss[part, :] * (gradient + linear[part, :])
                z = jnp.minimum(jnp.maximum(value, low[part, :]), high[part, :])
                u = value - z
                mz[0, part, :] = z
                mu[0, part, :] = u
                xb[part, :] = (z - u).astype(BF16)
                return (sums[0] + folded(z * z + u * u),)
            z0, u0 = (mz[0, part, :], mu[0, part, :]) if it == 1 else (sz[part, :], su[part, :])
            value = base[part, :] - ss[part, :] * gradient
            z = jnp.minimum(jnp.maximum(value, low[part, :]), high[part, :])
            u = value - z
            mz[it, part, :] = z
            mu[it, part, :] = u
            dz, du = z - z0, u - u0
            if it < ITERS - 1:
                cz[it - 1, part, :] = dz
                cu[it - 1, part, :] = du
            out = []
            for j in range(it):
                pz, pu = (
                    (mz[0, part, :], mu[0, part, :])
                    if j == 0
                    else (cz[j - 1, part, :], cu[j - 1, part, :])
                )
                out.append(sums[j] + folded(pz * dz + pu * du))
            out.append(sums[it] + folded(dz * dz + du * du))
            return tuple(out)

        zero = jnp.zeros((8, s), F32)
        sums = lax.fori_loop(0, n // CHUNK, mapped, (zero,) * (it + 1))
        sums = [jnp.sum(item, axis=0, keepdims=True) for item in sums]
        if it == 0:
            first = sums[0]
            continue
        shared = ([first] if it == 1 else []) + sums
        ga = gas[it - 1]
        for i in range(len(shared)):
            ga[me, pl.ds(i, 1), :] = shared[i]
        everyone(ga.at[me], ga.at[me], 4)
        arrived(ga.at[pl.ds(0, devices - 1)], 4)
        total = jnp.sum(ga[...], axis=0)
        left(ga.at[pl.ds(0, devices - 1)], 4)
        lines = [total[i : i + 1, :] for i in range(len(shared))]
        if it == 1:
            gram = [[lines[0]]]
            lines = lines[1:]
        for i in range(it):
            gram[i].append(lines[i])
        gram.append(lines)
        alpha = mix_weights(gram)

        def combined(i, carry):
            part = pl.ds(pl.multiple_of(i * CHUNK, CHUNK), CHUNK)
            z = alpha[0] * mz[0, part, :]
            u = alpha[0] * mu[0, part, :]
            for j in range(1, it + 1):
                z = z + alpha[j] * mz[j, part, :]
                u = u + alpha[j] * mu[j, part, :]
            z = jnp.minimum(jnp.maximum(z, low[part, :]), high[part, :])
            if it < ITERS - 1:
                sz[part, :] = z
                su[part, :] = u
                xb[part, :] = (z - u).astype(BF16)
            else:
                z_hbm[part, :] = z
                u_hbm[part, :] = u
            return carry

        lax.fori_loop(0, n // CHUNK, combined, 0)


def per_device(devices, design_matrix, targets, linear, diagonal, lower_code, upper_code):
    rows, n = design_matrix.shape
    s = linear.shape[1]
    quarters = devices // 2 // WINDOW
    block = rows // (2 * WINDOW)
    others = 2 * WINDOW - 1
    full = pltpu.VMEM((n, s), F32)
    hbm = pl.BlockSpec(memory_space=pl.ANY)
    return pl.pallas_call(
        functools.partial(kernel, devices),
        out_shape=(pltpu.VMEM((n, s), F32),) * 2,
        in_specs=[hbm] * 6,
        out_specs=(pl.BlockSpec(memory_space=pltpu.VMEM),) * 2,
        scratch_shapes=[
            pltpu.VMEM((rows, n), BF16),
            pltpu.VMEM((n, rows), BF16),
            full,
            pltpu.VMEM((n // 128, 128), F32),
            pltpu.VMEM((2, n, s), jnp.int32),
            full,
            full,
            full,
            full,
            pltpu.VMEM((ITERS, n, s), F32),
            pltpu.VMEM((ITERS, n, s), F32),
            pltpu.VMEM((ITERS - 2, n, s), F32),
            pltpu.VMEM((ITERS - 2, n, s), F32),
            full,
            full,
            full,
            pltpu.VMEM((n, s), BF16),
            pltpu.VMEM((rows, s), F32),
            pltpu.VMEM((rows, s), SENT_A),
            pltpu.VMEM((rows, s), F32),
            pltpu.VMEM((others, block, s), SENT_A),
            pltpu.VMEM((quarters, block, s), SENT_B),
            pltpu.VMEM((2, block, s), F32),
            pltpu.VMEM((block, s), F32),
            pltpu.VMEM((rows, s), BF16),
            pltpu.VMEM((block, s), F32),
            pltpu.VMEM((devices, 3, s), F32),
            pltpu.VMEM((devices, 3, s), F32),
            pltpu.VMEM((devices, 4, s), F32),
            pltpu.SemaphoreType.DMA((6,)),
            pltpu.SemaphoreType.DMA((2,)),
            pltpu.SemaphoreType.DMA((5,)),
            pltpu.SemaphoreType.DMA((5,)),
        ],
        compiler_params=pltpu.CompilerParams(
            collective_id=0, has_side_effects=True, vmem_limit_bytes=56 * 1024 * 1024
        ),
        name="admm",
    )(
        design_matrix,
        targets,
        linear,
        diagonal.reshape(n // 128, 128),
        lower_code,
        upper_code,
    )


def solution(mesh):
    in_specs = (
        P("groups", "row"),
        P(("groups", "row"), None),
        P(("groups", "row"), None),
        P(("groups", "row")),
        P(("groups", "row"), None),
        P(("groups", "row"), None),
    )
    out_specs = (P(("groups", "row"), None), P(("groups", "row"), None))
    return jax.shard_map(
        functools.partial(per_device, mesh.shape["row"]),
        mesh=mesh,
        in_specs=in_specs,
        out_specs=out_specs,
        check_vma=False,
    )
```

```python
import functools

import jax
import jax.numpy as jnp
from jax import lax
from jax.experimental import pallas as pl
from jax.experimental.pallas import tpu as pltpu
from jax.sharding import PartitionSpec as P

ITERS = 4
WINDOW = 4
CHUNK = 1024
rho_plus_lip = 7.0
F32, BF16 = jnp.float32, jnp.bfloat16
SENT_A, SENT_B = jnp.bfloat16, jnp.bfloat16


def solve_small(matrix, rhs):
    count = len(rhs)
    table = [list(line) for line in matrix]
    right = list(rhs)
    inverse = []
    for p in range(count):
        inverse.append(1.0 / table[p][p])
        for i in range(p + 1, count):
            factor = table[i][p] * inverse[p]
            for j in range(p + 1, count):
                table[i][j] = table[i][j] - factor * table[p][j]
            right[i] = right[i] - factor * right[p]
    result = [None] * count
    for i in reversed(range(count)):
        total = right[i]
        for j in range(i + 1, count):
            total = total - table[i][j] * result[j]
        result[i] = total * inverse[i]
    return result


def mix_weights(gram):
    count = len(gram)
    trace = gram[0][0]
    for i in range(1, count):
        trace = trace + gram[i][i]
    shift = 0.01 * trace / count + 1e-06
    matrix = [[gram[i][j] + (shift if i == j else 0.0) for j in range(count)] for i in range(count)]
    solved = solve_small(matrix, [jnp.ones_like(trace)] * count)
    total = solved[0]
    for i in range(1, count):
        total = total + solved[i]
    inverse = 1.0 / total
    return [item * inverse for item in solved]


def folded(value):
    return jnp.sum(value.reshape(-1, 8, value.shape[-1]), axis=0)


def kernel(
    devices,
    a_hbm, targets_hbm, linear_hbm, diagonal_hbm, lower_hbm, upper_hbm,
    z_hbm, u_hbm,
    a, a_t, linear, diagonal, code, low, high, dd, ss,
    mz, mu, cz, cu, sz, su, base, xb, pf, pb, known_a, ra, wb, known_b, window, m, targets, ga_1, ga_2, ga_3,
    load_sem, out_sem, send_sem, recv_sem,
):
    chips = devices // 2
    quarters = chips // WINDOW
    rows, n = a.shape
    block = rows // (2 * WINDOW)
    piece = block // quarters
    s = linear.shape[1]
    me = lax.axis_index("row")
    chip, core = me // 2, me % 2
    spot, quarter = chip % WINDOW, chip // WINDOW
    own = pl.multiple_of((2 * spot + core) * block, block)
    toward = 2 - 4 * core

    def at(offset, which):
        return 2 * ((chip + offset + chips) % chips) + which

    def owned_by(offset, which):
        return pl.multiple_of((2 * ((chip + offset + chips) % WINDOW) + which) * block, block)

    served = [at(-2, 0), at(2, 1)]
    for offset in (1, -1):
        for which in (0, 1):
            served.append(at(offset, which))
    served.append(at(0, 1 - core))
    def everyone(source, target, arrival):
        def chips_away(i, carry):
            away = (chips // 2 - (i + 1) // 2) * (1 - 2 * ((i + 1) % 2))
            for which in (0, 1):
                send(source, target, at(away, which), arrival, arrival)
            return carry

        lax.fori_loop(0, chips - 1, chips_away, 0)
        send(source, target, at(0, 1 - core), arrival, arrival)

    def left(buffer, index):
        pltpu.make_async_remote_copy(
            src_ref=buffer,
            dst_ref=buffer,
            send_sem=send_sem.at[index],
            recv_sem=recv_sem.at[0],
            device_id={"row": at(0, 1 - core)},
            device_id_type=pl.DeviceIdType.MESH,
        ).wait_send()

    sharers = [at(WINDOW * i, core) for i in range(1, quarters)]

    def send(source, target, device, index, arrival):
        copy = pltpu.make_async_remote_copy(
            src_ref=source,
            dst_ref=target,
            send_sem=send_sem.at[index],
            recv_sem=recv_sem.at[arrival],
            device_id={"row": device},
            device_id_type=pl.DeviceIdType.MESH,
        )
        copy.start()
        return copy

    def arrived(buffer, arrival):
        pltpu.make_async_remote_copy(
            src_ref=buffer,
            dst_ref=buffer,
            send_sem=send_sem.at[0],
            recv_sem=recv_sem.at[arrival],
            device_id={"row": at(0, 1 - core)},
            device_id_type=pl.DeviceIdType.MESH,
        ).wait_recv()

    def load(source, target, index):
        copy = pltpu.make_async_copy(source, target, load_sem.at[index])
        copy.start()
        return copy

    barrier = pltpu.get_barrier_semaphore()

    def greet(i, carry):
        away = (devices // 2 - (i + 1) // 2) * (1 - 2 * ((i + 1) % 2))
        pl.semaphore_signal(
            barrier,
            inc=1,
            device_id={"row": (me + away + devices) % devices},
            device_id_type=pl.DeviceIdType.MESH,
        )
        return carry

    lax.fori_loop(0, devices - 1, greet, 0)

    share = pl.ds(pl.multiple_of(quarter * piece, piece), piece)
    load_targets = load(targets_hbm, targets.at[share], 0)

    def load_a(i, carry):
        place, part = i // quarters, i % quarters
        source = pl.multiple_of((part * 2 * WINDOW + place) * piece, piece)
        target = pl.multiple_of(i * piece, piece)
        pltpu.make_async_copy(
            a_hbm.at[pl.ds(source, piece)], a.at[pl.ds(target, piece)], load_sem.at[1]
        ).start()
        return carry

    lax.fori_loop(0, 2 * WINDOW * quarters, load_a, 0)
    loads = [
        load(diagonal_hbm, diagonal, 2),
        load(lower_hbm, code.at[0], 3),
        load(upper_hbm, code.at[1], 4),
        load(linear_hbm, linear, 5),
    ]

    shown = pl.ds(pl.multiple_of(own + quarter * piece, piece), piece)
    load_targets.wait()
    m[shown, :] = (0.0 - targets[share, :]).astype(BF16)
    pl.semaphore_wait(barrier, devices - 1)
    everyone(m.at[shown], m.at[shown], 3)
    for device in sharers:
        send(targets.at[share], targets.at[share], device, 0, 0)

    pltpu.make_async_copy(a_hbm, a, load_sem.at[1]).wait()
    for copy in loads:
        copy.wait()

    def prepare(i, carry):
        part = pl.ds(pl.multiple_of(i * 128, 128), 128)
        a_t[part, :] = jnp.transpose(a[:, part])
        d = jnp.transpose(jnp.broadcast_to(diagonal[pl.ds(i, 1), :], (128, 128)))
        dd[part, :] = d
        ss[part, :] = 1.0 / (rho_plus_lip + d)
        low[part, :] = code[0, part, :].astype(F32) * (1.0 / 64.0)
        high[part, :] = code[1, part, :].astype(F32) * (1.0 / 64.0)
        return carry

    lax.fori_loop(0, n // 128, prepare, 0)

    arrived(m.at[pl.ds(0, rows - piece)], 3)
    left(m.at[pl.ds(0, rows - piece)], 3)

    gas = [ga_1, ga_2, ga_3]
    gram = []
    first = None
    for it in range(ITERS):
        mine = pl.ds(own, block)
        if it > 0:
            def multiplied(i, carry):
                offset = jnp.where(i == 0, toward, jnp.where(i == 3, 0, 3 - 2 * i))
                part = pl.ds(pl.multiple_of(owned_by(offset, 0), 2 * block), 2 * block)
                product = jnp.dot(a[part, :], xb[...], preferred_element_type=F32)
                pf[part, :] = product
                if it == 1:
                    rounded = product.astype(SENT_A)
                    known_a[part, :] = rounded.astype(F32)
                else:
                    known = known_a[part, :]
                    rounded = (product - known).astype(SENT_A)
                    known_a[part, :] = known + rounded.astype(F32)
                pb[part, :] = rounded

                @pl.when(i < WINDOW - 1)
                def _():
                    for which in (0, 1):
                        send(
                            pb.at[pl.ds(owned_by(offset, which), block)],
                            ra.at[2 * ((i + 2) % 3) + 1 + core],
                            at(offset, which),
                            1,
                            1,
                        )

                return carry

            def based(i, carry):
                part = pl.ds(pl.multiple_of(i * CHUNK, CHUNK), CHUNK)
                z0, u0 = (mz[0, part, :], mu[0, part, :]) if it == 1 else (sz[part, :], su[part, :])
                point = z0 - u0
                base[part, :] = z0 - ss[part, :] * (dd[part, :] * point + linear[part, :])
                return carry

            lax.fori_loop(0, WINDOW, multiplied, 0)
            send(pb.at[pl.ds(owned_by(0, 1 - core), block)], ra.at[0], at(0, 1 - core), 1, 1)
            lax.fori_loop(0, n // CHUNK, based, 0)
            arrived(ra, 1)
            total = ra[0].astype(F32)
            for i in range(1, len(served)):
                total = total + ra[i].astype(F32)
            if it > 1:
                total = total + window[...]
            window[...] = total
            total = total + pf[mine, :]
            if it > 1:
                total = total - known_b[0]
            rounded = total.astype(SENT_B)
            wb[quarter] = rounded
            known_b[0] = rounded.astype(F32) + (known_b[0] if it > 1 else 0.0)
            for device in sharers:
                send(wb.at[quarter], wb.at[quarter], device, 2, 2)
            left(ra, 1)
            arrived(wb.at[pl.ds(0, quarters - 1)], 2)
            total = wb[0].astype(F32)
            for i in range(1, quarters):
                total = total + wb[i].astype(F32)
            if it > 1:
                total = total + known_b[1]
            known_b[1] = total
            if it == 1:
                arrived(targets.at[pl.ds(0, (quarters - 1) * piece)], 0)
                left(targets.at[pl.ds(0, (quarters - 1) * piece)], 0)
            m[mine, :] = (total - targets[...]).astype(BF16)
            for device in served:
                send(m.at[mine], m.at[mine], device, 3, 3)
            left(wb.at[pl.ds(0, quarters - 1)], 2)
            arrived(m.at[pl.ds(0, rows - block)], 3)
            left(m.at[pl.ds(0, rows - block)], 3)

        def mapped(i, sums):
            part = pl.ds(pl.multiple_of(i * CHUNK, CHUNK), CHUNK)
            gradient = jnp.dot(a_t[part, :], m[...], preferred_element_type=F32)
            if it == 0:
                value = -ss[part, :] * (gradient + linear[part, :])
                z = jnp.minimum(jnp.maximum(value, low[part, :]), high[part, :])
                u = value - z
                mz[0, part, :] = z
                mu[0, part, :] = u
                xb[part, :] = (z - u).astype(BF16)
                return (sums[0] + folded(z * z + u * u),)
            z0, u0 = (mz[0, part, :], mu[0, part, :]) if it == 1 else (sz[part, :], su[part, :])
            value = base[part, :] - ss[part, :] * gradient
            z = jnp.minimum(jnp.maximum(value, low[part, :]), high[part, :])
            u = value - z
            mz[it, part, :] = z
            mu[it, part, :] = u
            dz, du = z - z0, u - u0
            if it < ITERS - 1:
                cz[it - 1, part, :] = dz
                cu[it - 1, part, :] = du
            out = []
            for j in range(it):
                pz, pu = (
                    (mz[0, part, :], mu[0, part, :])
                    if j == 0
                    else (cz[j - 1, part, :], cu[j - 1, part, :])
                )
                out.append(sums[j] + folded(pz * dz + pu * du))
            out.append(sums[it] + folded(dz * dz + du * du))
            return tuple(out)

        zero = jnp.zeros((8, s), F32)
        sums = lax.fori_loop(0, n // CHUNK, mapped, (zero,) * (it + 1))
        sums = [jnp.sum(item, axis=0, keepdims=True) for item in sums]
        if it == 0:
            first = sums[0]
            continue
        shared = ([first] if it == 1 else []) + sums
        ga = gas[it - 1]
        for i in range(len(shared)):
            ga[me, pl.ds(i, 1), :] = shared[i]
        everyone(ga.at[me], ga.at[me], 4)
        arrived(ga.at[pl.ds(0, devices - 1)], 4)
        total = jnp.sum(ga[...], axis=0)
        left(ga.at[pl.ds(0, devices - 1)], 4)
        lines = [total[i : i + 1, :] for i in range(len(shared))]
        if it == 1:
            gram = [[lines[0]]]
            lines = lines[1:]
        for i in range(it):
            gram[i].append(lines[i])
        gram.append(lines)
        alpha = mix_weights(gram)

        def combined(i, carry):
            part = pl.ds(pl.multiple_of(i * CHUNK, CHUNK), CHUNK)
            z = alpha[0] * mz[0, part, :]
            u = alpha[0] * mu[0, part, :]
            for j in range(1, it + 1):
                z = z + alpha[j] * mz[j, part, :]
                u = u + alpha[j] * mu[j, part, :]
            z = jnp.minimum(jnp.maximum(z, low[part, :]), high[part, :])
            if it < ITERS - 1:
                sz[part, :] = z
                su[part, :] = u
                xb[part, :] = (z - u).astype(BF16)
            else:
                z_hbm[part, :] = z
                u_hbm[part, :] = u
            return carry

        lax.fori_loop(0, n // CHUNK, combined, 0)


def per_device(devices, design_matrix, targets, linear, diagonal, lower_code, upper_code):
    rows, n = design_matrix.shape
    s = linear.shape[1]
    quarters = devices // 2 // WINDOW
    block = rows // (2 * WINDOW)
    others = 2 * WINDOW - 1
    full = pltpu.VMEM((n, s), F32)
    hbm = pl.BlockSpec(memory_space=pl.ANY)
    return pl.pallas_call(
        functools.partial(kernel, devices),
        out_shape=(pltpu.VMEM((n, s), F32),) * 2,
        in_specs=[hbm] * 6,
        out_specs=(pl.BlockSpec(memory_space=pltpu.VMEM),) * 2,
        scratch_shapes=[
            pltpu.VMEM((rows, n), BF16),
            pltpu.VMEM((n, rows), BF16),
            full,
            pltpu.VMEM((n // 128, 128), F32),
            pltpu.VMEM((2, n, s), jnp.int32),
            full,
            full,
            full,
            full,
            pltpu.VMEM((ITERS, n, s), F32),
            pltpu.VMEM((ITERS, n, s), F32),
            pltpu.VMEM((ITERS - 2, n, s), F32),
            pltpu.VMEM((ITERS - 2, n, s), F32),
            full,
            full,
            full,
            pltpu.VMEM((n, s), BF16),
            pltpu.VMEM((rows, s), F32),
            pltpu.VMEM((rows, s), SENT_A),
            pltpu.VMEM((rows, s), F32),
            pltpu.VMEM((others, block, s), SENT_A),
            pltpu.VMEM((quarters, block, s), SENT_B),
            pltpu.VMEM((2, block, s), F32),
            pltpu.VMEM((block, s), F32),
            pltpu.VMEM((rows, s), BF16),
            pltpu.VMEM((block, s), F32),
            pltpu.VMEM((devices, 3, s), F32),
            pltpu.VMEM((devices, 3, s), F32),
            pltpu.VMEM((devices, 4, s), F32),
            pltpu.SemaphoreType.DMA((6,)),
            pltpu.SemaphoreType.DMA((2,)),
            pltpu.SemaphoreType.DMA((5,)),
            pltpu.SemaphoreType.DMA((5,)),
        ],
        compiler_params=pltpu.CompilerParams(
            collective_id=0, has_side_effects=True, vmem_limit_bytes=56 * 1024 * 1024
        ),
        name="admm",
    )(
        design_matrix,
        targets,
        linear,
        diagonal.reshape(n // 128, 128),
        lower_code,
        upper_code,
    )


def solution(mesh):
    in_specs = (
        P("groups", "row"),
        P(("groups", "row"), None),
        P(("groups", "row"), None),
        P(("groups", "row")),
        P(("groups", "row"), None),
        P(("groups", "row"), None),
    )
    out_specs = (P(("groups", "row"), None), P(("groups", "row"), None))
    return jax.shard_map(
        functools.partial(per_device, mesh.shape["row"]),
        mesh=mesh,
        in_specs=in_specs,
        out_specs=out_specs,
        check_vma=False,
    )
```

```python
import functools

import jax
import jax.numpy as jnp
from jax import lax
from jax.experimental import pallas as pl
from jax.experimental.pallas import tpu as pltpu
from jax.sharding import PartitionSpec as P

ITERS = 4
WINDOW = 4
CHUNK = 1024
rho_plus_lip = 7.0
F32, BF16 = jnp.float32, jnp.bfloat16
SENT_A, SENT_B = jnp.bfloat16, jnp.bfloat16


def solve_small(matrix, rhs):
    count = len(rhs)
    table = [list(line) for line in matrix]
    right = list(rhs)
    inverse = []
    for p in range(count):
        inverse.append(1.0 / table[p][p])
        for i in range(p + 1, count):
            factor = table[i][p] * inverse[p]
            for j in range(p + 1, count):
                table[i][j] = table[i][j] - factor * table[p][j]
            right[i] = right[i] - factor * right[p]
    result = [None] * count
    for i in reversed(range(count)):
        total = right[i]
        for j in range(i + 1, count):
            total = total - table[i][j] * result[j]
        result[i] = total * inverse[i]
    return result


def mix_weights(gram):
    count = len(gram)
    trace = gram[0][0]
    for i in range(1, count):
        trace = trace + gram[i][i]
    shift = 0.01 * trace / count + 1e-06
    matrix = [[gram[i][j] + (shift if i == j else 0.0) for j in range(count)] for i in range(count)]
    solved = solve_small(matrix, [jnp.ones_like(trace)] * count)
    total = solved[0]
    for i in range(1, count):
        total = total + solved[i]
    inverse = 1.0 / total
    return [item * inverse for item in solved]


def folded(value):
    return jnp.sum(value.reshape(-1, 8, value.shape[-1]), axis=0)


def kernel(
    devices,
    a_hbm, targets_hbm, linear_hbm, diagonal_hbm, lower_hbm, upper_hbm,
    z_hbm, u_hbm,
    a, a_t, linear, diagonal, code, low, high, dd, ss,
    mz, mu, cz, cu, sz, su, base, xb, pf, pb, known_a, ra, wb, known_b, window, m, targets, ga_1, ga_2, ga_3,
    load_sem, out_sem, send_sem, recv_sem,
):
    chips = devices // 2
    quarters = chips // WINDOW
    rows, n = a.shape
    block = rows // (2 * WINDOW)
    piece = block // quarters
    s = linear.shape[1]
    me = lax.axis_index("row")
    chip, core = me // 2, me % 2
    spot, quarter = chip % WINDOW, chip // WINDOW
    own = pl.multiple_of((2 * spot + core) * block, block)
    toward = 2 - 4 * core

    def at(offset, which):
        return 2 * ((chip + offset + chips) % chips) + which

    def owned_by(offset, which):
        return pl.multiple_of((2 * ((chip + offset + chips) % WINDOW) + which) * block, block)

    served = [at(-2, 0), at(2, 1)]
    for offset in (1, -1):
        for which in (0, 1):
            served.append(at(offset, which))
    served.append(at(0, 1 - core))
    def everyone(source, target, arrival):
        def chips_away(i, carry):
            away = (chips // 2 - (i + 1) // 2) * (1 - 2 * ((i + 1) % 2))
            for which in (0, 1):
                send(source, target, at(away, which), arrival, arrival)
            return carry

        lax.fori_loop(0, chips - 1, chips_away, 0)
        send(source, target, at(0, 1 - core), arrival, arrival)

    def left(buffer, index):
        pltpu.make_async_remote_copy(
            src_ref=buffer,
            dst_ref=buffer,
            send_sem=send_sem.at[index],
            recv_sem=recv_sem.at[0],
            device_id={"row": at(0, 1 - core)},
            device_id_type=pl.DeviceIdType.MESH,
        ).wait_send()

    sharers = [at(WINDOW * i, core) for i in (2, 1, 3)]

    def send(source, target, device, index, arrival):
        copy = pltpu.make_async_remote_copy(
            src_ref=source,
            dst_ref=target,
            send_sem=send_sem.at[index],
            recv_sem=recv_sem.at[arrival],
            device_id={"row": device},
            device_id_type=pl.DeviceIdType.MESH,
        )
        copy.start()
        return copy

    def arrived(buffer, arrival):
        pltpu.make_async_remote_copy(
            src_ref=buffer,
            dst_ref=buffer,
            send_sem=send_sem.at[0],
            recv_sem=recv_sem.at[arrival],
            device_id={"row": at(0, 1 - core)},
            device_id_type=pl.DeviceIdType.MESH,
        ).wait_recv()

    def load(source, target, index):
        copy = pltpu.make_async_copy(source, target, load_sem.at[index])
        copy.start()
        return copy

    barrier = pltpu.get_barrier_semaphore()

    def greet(i, carry):
        away = (devices // 2 - (i + 1) // 2) * (1 - 2 * ((i + 1) % 2))
        pl.semaphore_signal(
            barrier,
            inc=1,
            device_id={"row": (me + away + devices) % devices},
            device_id_type=pl.DeviceIdType.MESH,
        )
        return carry

    lax.fori_loop(0, devices - 1, greet, 0)

    share = pl.ds(pl.multiple_of(quarter * piece, piece), piece)
    load_targets = load(targets_hbm, targets.at[share], 0)

    def load_a(i, carry):
        place, part = i // quarters, i % quarters
        source = pl.multiple_of((part * 2 * WINDOW + place) * piece, piece)
        target = pl.multiple_of(i * piece, piece)
        pltpu.make_async_copy(
            a_hbm.at[pl.ds(source, piece)], a.at[pl.ds(target, piece)], load_sem.at[1]
        ).start()
        return carry

    lax.fori_loop(0, 2 * WINDOW * quarters, load_a, 0)
    loads = [
        load(diagonal_hbm, diagonal, 2),
        load(lower_hbm, code.at[0], 3),
        load(upper_hbm, code.at[1], 4),
        load(linear_hbm, linear, 5),
    ]

    shown = pl.ds(pl.multiple_of(own + quarter * piece, piece), piece)
    load_targets.wait()
    m[shown, :] = (0.0 - targets[share, :]).astype(BF16)
    pl.semaphore_wait(barrier, devices - 1)
    everyone(m.at[shown], m.at[shown], 3)
    for device in sharers:
        send(targets.at[share], targets.at[share], device, 0, 0)

    pltpu.make_async_copy(a_hbm, a, load_sem.at[1]).wait()
    for copy in loads:
        copy.wait()

    def prepare(i, carry):
        part = pl.ds(pl.multiple_of(i * 128, 128), 128)
        a_t[part, :] = jnp.transpose(a[:, part])
        d = jnp.transpose(jnp.broadcast_to(diagonal[pl.ds(i, 1), :], (128, 128)))
        dd[part, :] = d
        ss[part, :] = 1.0 / (rho_plus_lip + d)
        low[part, :] = code[0, part, :].astype(F32) * (1.0 / 64.0)
        high[part, :] = code[1, part, :].astype(F32) * (1.0 / 64.0)
        return carry

    lax.fori_loop(0, n // 128, prepare, 0)

    arrived(m.at[pl.ds(0, rows - piece)], 3)
    left(m.at[pl.ds(0, rows - piece)], 3)

    gas = [ga_1, ga_2, ga_3]
    gram = []
    first = None
    for it in range(ITERS):
        mine = pl.ds(own, block)
        if it > 0:
            def multiplied(i, carry):
                offset = jnp.where(i == 0, toward, jnp.where(i == 3, 0, 3 - 2 * i))
                part = pl.ds(pl.multiple_of(owned_by(offset, 0), 2 * block), 2 * block)
                product = jnp.dot(a[part, :], xb[...], preferred_element_type=F32)
                pf[part, :] = product
                if it == 1:
                    rounded = product.astype(SENT_A)
                    known_a[part, :] = rounded.astype(F32)
                else:
                    known = known_a[part, :]
                    rounded = (product - known).astype(SENT_A)
                    known_a[part, :] = known + rounded.astype(F32)
                pb[part, :] = rounded

                @pl.when(i < WINDOW - 1)
                def _():
                    for which in (0, 1):
                        send(
                            pb.at[pl.ds(owned_by(offset, which), block)],
                            ra.at[2 * ((i + 2) % 3) + 1 + core],
                            at(offset, which),
                            1,
                            1,
                        )

                return carry

            def based(i, carry):
                part = pl.ds(pl.multiple_of(i * CHUNK, CHUNK), CHUNK)
                z0, u0 = (mz[0, part, :], mu[0, part, :]) if it == 1 else (sz[part, :], su[part, :])
                point = z0 - u0
                base[part, :] = z0 - ss[part, :] * (dd[part, :] * point + linear[part, :])
                return carry

            lax.fori_loop(0, WINDOW, multiplied, 0)
            send(pb.at[pl.ds(owned_by(0, 1 - core), block)], ra.at[0], at(0, 1 - core), 1, 1)
            arrived(ra, 1)
            total = ra[0].astype(F32)
            for i in range(1, len(served)):
                total = total + ra[i].astype(F32)
            if it > 1:
                total = total + window[...]
            window[...] = total
            total = total + pf[mine, :]
            if it > 1:
                total = total - known_b[0]
            rounded = total.astype(SENT_B)
            wb[quarter] = rounded
            known_b[0] = rounded.astype(F32) + (known_b[0] if it > 1 else 0.0)
            send(wb.at[quarter], wb.at[quarter], sharers[0], 2, 2)
            lax.fori_loop(0, n // CHUNK, based, 0)
            for device in sharers[1:]:
                send(wb.at[quarter], wb.at[quarter], device, 2, 2)
            left(ra, 1)
            arrived(wb.at[pl.ds(0, quarters - 1)], 2)
            total = wb[0].astype(F32)
            for i in range(1, quarters):
                total = total + wb[i].astype(F32)
            if it > 1:
                total = total + known_b[1]
            known_b[1] = total
            if it == 1:
                arrived(targets.at[pl.ds(0, (quarters - 1) * piece)], 0)
                left(targets.at[pl.ds(0, (quarters - 1) * piece)], 0)
            m[mine, :] = (total - targets[...]).astype(BF16)
            for device in served:
                send(m.at[mine], m.at[mine], device, 3, 3)
            left(wb.at[pl.ds(0, quarters - 1)], 2)
            arrived(m.at[pl.ds(0, rows - block)], 3)
            left(m.at[pl.ds(0, rows - block)], 3)

        def mapped(i, sums):
            part = pl.ds(pl.multiple_of(i * CHUNK, CHUNK), CHUNK)
            gradient = jnp.dot(a_t[part, :], m[...], preferred_element_type=F32)
            if it == 0:
                value = -ss[part, :] * (gradient + linear[part, :])
                z = jnp.minimum(jnp.maximum(value, low[part, :]), high[part, :])
                u = value - z
                mz[0, part, :] = z
                mu[0, part, :] = u
                xb[part, :] = (z - u).astype(BF16)
                return (sums[0] + folded(z * z + u * u),)
            z0, u0 = (mz[0, part, :], mu[0, part, :]) if it == 1 else (sz[part, :], su[part, :])
            value = base[part, :] - ss[part, :] * gradient
            z = jnp.minimum(jnp.maximum(value, low[part, :]), high[part, :])
            u = value - z
            mz[it, part, :] = z
            mu[it, part, :] = u
            dz, du = z - z0, u - u0
            if it < ITERS - 1:
                cz[it - 1, part, :] = dz
                cu[it - 1, part, :] = du
            out = []
            for j in range(it):
                pz, pu = (
                    (mz[0, part, :], mu[0, part, :])
                    if j == 0
                    else (cz[j - 1, part, :], cu[j - 1, part, :])
                )
                out.append(sums[j] + folded(pz * dz + pu * du))
            out.append(sums[it] + folded(dz * dz + du * du))
            return tuple(out)

        zero = jnp.zeros((8, s), F32)
        sums = lax.fori_loop(0, n // CHUNK, mapped, (zero,) * (it + 1))
        sums = [jnp.sum(item, axis=0, keepdims=True) for item in sums]
        if it == 0:
            first = sums[0]
            continue
        shared = ([first] if it == 1 else []) + sums
        ga = gas[it - 1]
        for i in range(len(shared)):
            ga[me, pl.ds(i, 1), :] = shared[i]
        everyone(ga.at[me], ga.at[me], 4)
        arrived(ga.at[pl.ds(0, devices - 1)], 4)
        total = jnp.sum(ga[...], axis=0)
        left(ga.at[pl.ds(0, devices - 1)], 4)
        lines = [total[i : i + 1, :] for i in range(len(shared))]
        if it == 1:
            gram = [[lines[0]]]
            lines = lines[1:]
        for i in range(it):
            gram[i].append(lines[i])
        gram.append(lines)
        alpha = mix_weights(gram)

        def combined(i, carry):
            part = pl.ds(pl.multiple_of(i * CHUNK, CHUNK), CHUNK)
            z = alpha[0] * mz[0, part, :]
            u = alpha[0] * mu[0, part, :]
            for j in range(1, it + 1):
                z = z + alpha[j] * mz[j, part, :]
                u = u + alpha[j] * mu[j, part, :]
            z = jnp.minimum(jnp.maximum(z, low[part, :]), high[part, :])
            if it < ITERS - 1:
                sz[part, :] = z
                su[part, :] = u
                xb[part, :] = (z - u).astype(BF16)
            else:
                z_hbm[part, :] = z
                u_hbm[part, :] = u
            return carry

        lax.fori_loop(0, n // CHUNK, combined, 0)


def per_device(devices, design_matrix, targets, linear, diagonal, lower_code, upper_code):
    rows, n = design_matrix.shape
    s = linear.shape[1]
    quarters = devices // 2 // WINDOW
    block = rows // (2 * WINDOW)
    others = 2 * WINDOW - 1
    full = pltpu.VMEM((n, s), F32)
    hbm = pl.BlockSpec(memory_space=pl.ANY)
    return pl.pallas_call(
        functools.partial(kernel, devices),
        out_shape=(pltpu.VMEM((n, s), F32),) * 2,
        in_specs=[hbm] * 6,
        out_specs=(pl.BlockSpec(memory_space=pltpu.VMEM),) * 2,
        scratch_shapes=[
            pltpu.VMEM((rows, n), BF16),
            pltpu.VMEM((n, rows), BF16),
            full,
            pltpu.VMEM((n // 128, 128), F32),
            pltpu.VMEM((2, n, s), jnp.int32),
            full,
            full,
            full,
            full,
            pltpu.VMEM((ITERS, n, s), F32),
            pltpu.VMEM((ITERS, n, s), F32),
            pltpu.VMEM((ITERS - 2, n, s), F32),
            pltpu.VMEM((ITERS - 2, n, s), F32),
            full,
            full,
            full,
            pltpu.VMEM((n, s), BF16),
            pltpu.VMEM((rows, s), F32),
            pltpu.VMEM((rows, s), SENT_A),
            pltpu.VMEM((rows, s), F32),
            pltpu.VMEM((others, block, s), SENT_A),
            pltpu.VMEM((quarters, block, s), SENT_B),
            pltpu.VMEM((2, block, s), F32),
            pltpu.VMEM((block, s), F32),
            pltpu.VMEM((rows, s), BF16),
            pltpu.VMEM((block, s), F32),
            pltpu.VMEM((devices, 3, s), F32),
            pltpu.VMEM((devices, 3, s), F32),
            pltpu.VMEM((devices, 4, s), F32),
            pltpu.SemaphoreType.DMA((6,)),
            pltpu.SemaphoreType.DMA((2,)),
            pltpu.SemaphoreType.DMA((5,)),
            pltpu.SemaphoreType.DMA((5,)),
        ],
        compiler_params=pltpu.CompilerParams(
            collective_id=0, has_side_effects=True, vmem_limit_bytes=56 * 1024 * 1024
        ),
        name="admm",
    )(
        design_matrix,
        targets,
        linear,
        diagonal.reshape(n // 128, 128),
        lower_code,
        upper_code,
    )


def solution(mesh):
    in_specs = (
        P("groups", "row"),
        P(("groups", "row"), None),
        P(("groups", "row"), None),
        P(("groups", "row")),
        P(("groups", "row"), None),
        P(("groups", "row"), None),
    )
    out_specs = (P(("groups", "row"), None), P(("groups", "row"), None))
    return jax.shard_map(
        functools.partial(per_device, mesh.shape["row"]),
        mesh=mesh,
        in_specs=in_specs,
        out_specs=out_specs,
        check_vma=False,
    )
```

```python
import functools

import jax
import jax.numpy as jnp
from jax import lax
from jax.experimental import pallas as pl
from jax.experimental.pallas import tpu as pltpu
from jax.sharding import PartitionSpec as P

ITERS = 4
WINDOW = 4
CHUNK = 1024
rho_plus_lip = 7.0
F32, BF16 = jnp.float32, jnp.bfloat16
SENT_A, SENT_B = jnp.bfloat16, jnp.bfloat16


def solve_small(matrix, rhs):
    count = len(rhs)
    table = [list(line) for line in matrix]
    right = list(rhs)
    inverse = []
    for p in range(count):
        inverse.append(1.0 / table[p][p])
        for i in range(p + 1, count):
            factor = table[i][p] * inverse[p]
            for j in range(p + 1, count):
                table[i][j] = table[i][j] - factor * table[p][j]
            right[i] = right[i] - factor * right[p]
    result = [None] * count
    for i in reversed(range(count)):
        total = right[i]
        for j in range(i + 1, count):
            total = total - table[i][j] * result[j]
        result[i] = total * inverse[i]
    return result


def mix_weights(gram):
    count = len(gram)
    trace = gram[0][0]
    for i in range(1, count):
        trace = trace + gram[i][i]
    shift = 0.01 * trace / count + 1e-06
    matrix = [[gram[i][j] + (shift if i == j else 0.0) for j in range(count)] for i in range(count)]
    solved = solve_small(matrix, [jnp.ones_like(trace)] * count)
    total = solved[0]
    for i in range(1, count):
        total = total + solved[i]
    inverse = 1.0 / total
    return [item * inverse for item in solved]


def folded(value):
    return jnp.sum(value.reshape(-1, 8, value.shape[-1]), axis=0)


def kernel(
    devices,
    a_hbm, targets_hbm, linear_hbm, diagonal_hbm, lower_hbm, upper_hbm,
    mz, mu, low, high, *rest,
):
    last, rest = rest[:ITERS], rest[ITERS:]
    (
        a,
        a_t,
        linear,
        diagonal,
        code,
        dd,
        ss,
        cz,
        cu,
        sz,
        su,
        base,
        xb,
        pf,
        pb,
        known_a,
        ra,
        wb,
        known_b,
        window,
        m,
        targets,
        ga_1,
        ga_2,
        ga_3,
        load_sem,
        send_sem,
        recv_sem,
    ) = rest
    chips = devices // 2
    quarters = chips // WINDOW
    rows, n = a.shape
    block = rows // (2 * WINDOW)
    piece = block // quarters
    s = linear.shape[1]
    me = lax.axis_index("row")
    chip, core = me // 2, me % 2
    spot, quarter = chip % WINDOW, chip // WINDOW
    own = pl.multiple_of((2 * spot + core) * block, block)
    toward = 2 - 4 * core

    def at(offset, which):
        return 2 * ((chip + offset + chips) % chips) + which

    def owned_by(offset, which):
        return pl.multiple_of((2 * ((chip + offset + chips) % WINDOW) + which) * block, block)

    served = [at(-2, 0), at(2, 1)]
    for offset in (1, -1):
        for which in (0, 1):
            served.append(at(offset, which))
    served.append(at(0, 1 - core))
    def everyone(source, target, arrival):
        def chips_away(i, carry):
            away = (chips // 2 - (i + 1) // 2) * (1 - 2 * ((i + 1) % 2))
            for which in (0, 1):
                send(source, target, at(away, which), arrival, arrival)
            return carry

        lax.fori_loop(0, chips - 1, chips_away, 0)
        send(source, target, at(0, 1 - core), arrival, arrival)

    def left(buffer, index):
        pltpu.make_async_remote_copy(
            src_ref=buffer,
            dst_ref=buffer,
            send_sem=send_sem.at[index],
            recv_sem=recv_sem.at[0],
            device_id={"row": at(0, 1 - core)},
            device_id_type=pl.DeviceIdType.MESH,
        ).wait_send()

    sharers = [at(WINDOW * i, core) for i in (2, 1, 3)]

    def send(source, target, device, index, arrival):
        copy = pltpu.make_async_remote_copy(
            src_ref=source,
            dst_ref=target,
            send_sem=send_sem.at[index],
            recv_sem=recv_sem.at[arrival],
            device_id={"row": device},
            device_id_type=pl.DeviceIdType.MESH,
        )
        copy.start()
        return copy

    def arrived(buffer, arrival):
        pltpu.make_async_remote_copy(
            src_ref=buffer,
            dst_ref=buffer,
            send_sem=send_sem.at[0],
            recv_sem=recv_sem.at[arrival],
            device_id={"row": at(0, 1 - core)},
            device_id_type=pl.DeviceIdType.MESH,
        ).wait_recv()

    def load(source, target, index):
        copy = pltpu.make_async_copy(source, target, load_sem.at[index])
        copy.start()
        return copy

    barrier = pltpu.get_barrier_semaphore()

    def greet(i, carry):
        away = (devices // 2 - (i + 1) // 2) * (1 - 2 * ((i + 1) % 2))
        pl.semaphore_signal(
            barrier,
            inc=1,
            device_id={"row": (me + away + devices) % devices},
            device_id_type=pl.DeviceIdType.MESH,
        )
        return carry

    lax.fori_loop(0, devices - 1, greet, 0)

    share = pl.ds(pl.multiple_of(quarter * piece, piece), piece)
    load_targets = load(targets_hbm, targets.at[share], 0)

    def load_a(i, carry):
        place, part = i // quarters, i % quarters
        source = pl.multiple_of((part * 2 * WINDOW + place) * piece, piece)
        target = pl.multiple_of(i * piece, piece)
        pltpu.make_async_copy(
            a_hbm.at[pl.ds(source, piece)], a.at[pl.ds(target, piece)], load_sem.at[1]
        ).start()
        return carry

    lax.fori_loop(0, 2 * WINDOW * quarters, load_a, 0)
    loads = [
        load(diagonal_hbm, diagonal, 2),
        load(lower_hbm, code.at[0], 3),
        load(upper_hbm, code.at[1], 4),
        load(linear_hbm, linear, 5),
    ]

    shown = pl.ds(pl.multiple_of(own + quarter * piece, piece), piece)
    load_targets.wait()
    m[shown, :] = (0.0 - targets[share, :]).astype(BF16)
    pl.semaphore_wait(barrier, devices - 1)
    everyone(m.at[shown], m.at[shown], 3)
    for device in sharers:
        send(targets.at[share], targets.at[share], device, 0, 0)

    pltpu.make_async_copy(a_hbm, a, load_sem.at[1]).wait()
    for copy in loads:
        copy.wait()

    def prepare(i, carry):
        part = pl.ds(pl.multiple_of(i * 128, 128), 128)
        a_t[part, :] = jnp.transpose(a[:, part])
        d = jnp.transpose(jnp.broadcast_to(diagonal[pl.ds(i, 1), :], (128, 128)))
        dd[part, :] = d
        ss[part, :] = 1.0 / (rho_plus_lip + d)
        low[part, :] = code[0, part, :].astype(F32) * (1.0 / 64.0)
        high[part, :] = code[1, part, :].astype(F32) * (1.0 / 64.0)
        return carry

    lax.fori_loop(0, n // 128, prepare, 0)

    arrived(m.at[pl.ds(0, rows - piece)], 3)
    left(m.at[pl.ds(0, rows - piece)], 3)

    gas = [ga_1, ga_2, ga_3]
    gram = []
    first = None
    for it in range(ITERS):
        mine = pl.ds(own, block)
        if it > 0:
            def multiplied(i, carry):
                offset = jnp.where(i == 0, toward, jnp.where(i == 3, 0, 3 - 2 * i))
                part = pl.ds(pl.multiple_of(owned_by(offset, 0), 2 * block), 2 * block)
                product = jnp.dot(a[part, :], xb[...], preferred_element_type=F32)
                pf[part, :] = product
                if it == 1:
                    rounded = product.astype(SENT_A)
                    known_a[part, :] = rounded.astype(F32)
                else:
                    known = known_a[part, :]
                    rounded = (product - known).astype(SENT_A)
                    known_a[part, :] = known + rounded.astype(F32)
                pb[part, :] = rounded

                @pl.when(i < WINDOW - 1)
                def _():
                    for which in (0, 1):
                        send(
                            pb.at[pl.ds(owned_by(offset, which), block)],
                            ra.at[2 * ((i + 2) % 3) + 1 + core],
                            at(offset, which),
                            1,
                            1,
                        )

                return carry

            def based(i, carry):
                part = pl.ds(pl.multiple_of(i * CHUNK, CHUNK), CHUNK)
                z0, u0 = (mz[0, part, :], mu[0, part, :]) if it == 1 else (sz[part, :], su[part, :])
                point = z0 - u0
                base[part, :] = z0 - ss[part, :] * (dd[part, :] * point + linear[part, :])
                return carry

            lax.fori_loop(0, WINDOW, multiplied, 0)
            send(pb.at[pl.ds(owned_by(0, 1 - core), block)], ra.at[0], at(0, 1 - core), 1, 1)
            arrived(ra, 1)
            total = ra[0].astype(F32)
            for i in range(1, len(served)):
                total = total + ra[i].astype(F32)
            if it > 1:
                total = total + window[...]
            window[...] = total
            total = total + pf[mine, :]
            if it > 1:
                total = total - known_b[0]
            rounded = total.astype(SENT_B)
            wb[quarter] = rounded
            known_b[0] = rounded.astype(F32) + (known_b[0] if it > 1 else 0.0)
            send(wb.at[quarter], wb.at[quarter], sharers[0], 2, 2)
            lax.fori_loop(0, n // CHUNK, based, 0)
            for device in sharers[1:]:
                send(wb.at[quarter], wb.at[quarter], device, 2, 2)
            left(ra, 1)
            arrived(wb.at[pl.ds(0, quarters - 1)], 2)
            total = wb[0].astype(F32)
            for i in range(1, quarters):
                total = total + wb[i].astype(F32)
            if it > 1:
                total = total + known_b[1]
            known_b[1] = total
            if it == 1:
                arrived(targets.at[pl.ds(0, (quarters - 1) * piece)], 0)
                left(targets.at[pl.ds(0, (quarters - 1) * piece)], 0)
            m[mine, :] = (total - targets[...]).astype(BF16)
            for device in served:
                send(m.at[mine], m.at[mine], device, 3, 3)
            left(wb.at[pl.ds(0, quarters - 1)], 2)
            arrived(m.at[pl.ds(0, rows - block)], 3)
            left(m.at[pl.ds(0, rows - block)], 3)

        def mapped(i, sums):
            part = pl.ds(pl.multiple_of(i * CHUNK, CHUNK), CHUNK)
            gradient = jnp.dot(a_t[part, :], m[...], preferred_element_type=F32)
            if it == 0:
                value = -ss[part, :] * (gradient + linear[part, :])
                z = jnp.minimum(jnp.maximum(value, low[part, :]), high[part, :])
                u = value - z
                mz[0, part, :] = z
                mu[0, part, :] = u
                xb[part, :] = (z - u).astype(BF16)
                return (sums[0] + folded(z * z + u * u),)
            z0, u0 = (mz[0, part, :], mu[0, part, :]) if it == 1 else (sz[part, :], su[part, :])
            value = base[part, :] - ss[part, :] * gradient
            past = [(z0, u0) if it == 1 else (mz[0, part, :], mu[0, part, :])]
            past += [(cz[j, part, :], cu[j, part, :]) for j in range(it - 1)]
            z = jnp.minimum(jnp.maximum(value, low[part, :]), high[part, :])
            u = value - z
            mz[it, part, :] = z
            mu[it, part, :] = u
            dz, du = z - z0, u - u0
            if it < ITERS - 1:
                cz[it - 1, part, :] = dz
                cu[it - 1, part, :] = du
            out = [sums[j] + folded(pz * dz + pu * du) for j, (pz, pu) in enumerate(past)]
            out.append(sums[it] + folded(dz * dz + du * du))
            return tuple(out)

        zero = jnp.zeros((8, s), F32)
        sums = lax.fori_loop(0, n // CHUNK, mapped, (zero,) * (it + 1))
        sums = [jnp.sum(item, axis=0, keepdims=True) for item in sums]
        if it == 0:
            first = sums[0]
            continue
        shared = ([first] if it == 1 else []) + sums
        ga = gas[it - 1]
        for i in range(len(shared)):
            ga[me, pl.ds(i, 1), :] = shared[i]
        everyone(ga.at[me], ga.at[me], 4)
        arrived(ga.at[pl.ds(0, devices - 1)], 4)
        total = jnp.sum(ga[...], axis=0)
        left(ga.at[pl.ds(0, devices - 1)], 4)
        lines = [total[i : i + 1, :] for i in range(len(shared))]
        if it == 1:
            gram = [[lines[0]]]
            lines = lines[1:]
        for i in range(it):
            gram[i].append(lines[i])
        gram.append(lines)
        alpha = mix_weights(gram)

        def combined(i, carry):
            part = pl.ds(pl.multiple_of(i * CHUNK, CHUNK), CHUNK)
            z = alpha[0] * mz[0, part, :]
            u = alpha[0] * mu[0, part, :]
            for j in range(1, it + 1):
                z = z + alpha[j] * mz[j, part, :]
                u = u + alpha[j] * mu[j, part, :]
            z = jnp.minimum(jnp.maximum(z, low[part, :]), high[part, :])
            sz[part, :] = z
            su[part, :] = u
            xb[part, :] = (z - u).astype(BF16)
            return carry

        if it == ITERS - 1:
            for j in range(it + 1):
                last[j][...] = alpha[j]
            break
        lax.fori_loop(0, n // CHUNK, combined, 0)


def per_device(devices, design_matrix, targets, linear, diagonal, lower_code, upper_code):
    rows, n = design_matrix.shape
    s = linear.shape[1]
    quarters = devices // 2 // WINDOW
    block = rows // (2 * WINDOW)
    others = 2 * WINDOW - 1
    full = pltpu.VMEM((n, s), F32)
    hbm = pl.BlockSpec(memory_space=pl.ANY)
    mz, mu, low, high, *alpha = pl.pallas_call(
        functools.partial(kernel, devices),
        out_shape=(
            pltpu.VMEM((ITERS, n, s), F32),
            pltpu.VMEM((ITERS, n, s), F32),
            pltpu.VMEM((n, s), F32),
            pltpu.VMEM((n, s), F32),
            *[pltpu.VMEM((1, s), F32)] * ITERS,
        ),
        in_specs=[hbm] * 6,
        out_specs=(pl.BlockSpec(memory_space=pltpu.VMEM),) * (4 + ITERS),
        scratch_shapes=[
            pltpu.VMEM((rows, n), BF16),
            pltpu.VMEM((n, rows), BF16),
            full,
            pltpu.VMEM((n // 128, 128), F32),
            pltpu.VMEM((2, n, s), jnp.int32),
            full,
            full,
            pltpu.VMEM((ITERS - 2, n, s), F32),
            pltpu.VMEM((ITERS - 2, n, s), F32),
            full,
            full,
            full,
            pltpu.VMEM((n, s), BF16),
            pltpu.VMEM((rows, s), F32),
            pltpu.VMEM((rows, s), SENT_A),
            pltpu.VMEM((rows, s), F32),
            pltpu.VMEM((others, block, s), SENT_A),
            pltpu.VMEM((quarters, block, s), SENT_B),
            pltpu.VMEM((2, block, s), F32),
            pltpu.VMEM((block, s), F32),
            pltpu.VMEM((rows, s), BF16),
            pltpu.VMEM((block, s), F32),
            pltpu.VMEM((devices, 3, s), F32),
            pltpu.VMEM((devices, 3, s), F32),
            pltpu.VMEM((devices, 4, s), F32),
            pltpu.SemaphoreType.DMA((6,)),
            pltpu.SemaphoreType.DMA((5,)),
            pltpu.SemaphoreType.DMA((5,)),
        ],
        compiler_params=pltpu.CompilerParams(
            collective_id=0, has_side_effects=True, vmem_limit_bytes=53 * 1024 * 1024
        ),
        name="admm",
    )(
        design_matrix,
        targets,
        linear,
        diagonal.reshape(n // 128, 128),
        lower_code,
        upper_code,
    )
    z, u = alpha[0] * mz[0], alpha[0] * mu[0]
    for j in range(1, ITERS):
        z, u = z + alpha[j] * mz[j], u + alpha[j] * mu[j]
    return jnp.minimum(jnp.maximum(z, low), high), u


def solution(mesh):
    in_specs = (
        P("groups", "row"),
        P(("groups", "row"), None),
        P(("groups", "row"), None),
        P(("groups", "row")),
        P(("groups", "row"), None),
        P(("groups", "row"), None),
    )
    out_specs = (P(("groups", "row"), None), P(("groups", "row"), None))
    return jax.shard_map(
        functools.partial(per_device, mesh.shape["row"]),
        mesh=mesh,
        in_specs=in_specs,
        out_specs=out_specs,
        check_vma=False,
    )
```

```python
import functools

import jax
import jax.numpy as jnp
from jax import lax
from jax.experimental import pallas as pl
from jax.experimental.pallas import tpu as pltpu
from jax.sharding import PartitionSpec as P

ITERS = 4
WINDOW = 4
CHUNK = 1024
rho_plus_lip = 7.0
F32, BF16 = jnp.float32, jnp.bfloat16
SENT_A, SENT_B = jnp.bfloat16, jnp.bfloat16


def solve_small(matrix, rhs):
    count = len(rhs)
    table = [list(line) for line in matrix]
    right = list(rhs)
    inverse = []
    for p in range(count):
        inverse.append(1.0 / table[p][p])
        for i in range(p + 1, count):
            factor = table[i][p] * inverse[p]
            for j in range(p + 1, count):
                table[i][j] = table[i][j] - factor * table[p][j]
            right[i] = right[i] - factor * right[p]
    result = [None] * count
    for i in reversed(range(count)):
        total = right[i]
        for j in range(i + 1, count):
            total = total - table[i][j] * result[j]
        result[i] = total * inverse[i]
    return result


def mix_weights(gram):
    count = len(gram)
    trace = gram[0][0]
    for i in range(1, count):
        trace = trace + gram[i][i]
    shift = 0.01 * trace / count + 1e-06
    matrix = [[gram[i][j] + (shift if i == j else 0.0) for j in range(count)] for i in range(count)]
    solved = solve_small(matrix, [jnp.ones_like(trace)] * count)
    total = solved[0]
    for i in range(1, count):
        total = total + solved[i]
    inverse = 1.0 / total
    return [item * inverse for item in solved]


def folded(value):
    return jnp.sum(value.reshape(-1, 8, value.shape[-1]), axis=0)


def kernel(
    devices,
    a_hbm, targets_hbm, linear_hbm, diagonal_hbm, lower_hbm, upper_hbm,
    mz, mu, low, high, *rest,
):
    last, rest = rest[:ITERS], rest[ITERS:]
    (
        a,
        a_t,
        linear,
        diagonal,
        code,
        dd,
        ss,
        cz,
        cu,
        sz,
        su,
        base,
        xb,
        pf,
        pb,
        known_a,
        ra,
        wb,
        known_b,
        window,
        m,
        targets,
        ga_1,
        ga_2,
        ga_3,
        load_sem,
        send_sem,
        recv_sem,
    ) = rest
    chips = devices // 2
    quarters = chips // WINDOW
    rows, n = a.shape
    block = rows // (2 * WINDOW)
    piece = block // quarters
    s = linear.shape[1]
    me = lax.axis_index("row")
    chip, core = me // 2, me % 2
    spot, quarter = chip % WINDOW, chip // WINDOW
    own = pl.multiple_of((2 * spot + core) * block, block)
    toward = 2 - 4 * core

    def at(offset, which):
        return 2 * ((chip + offset + chips) % chips) + which

    def owned_by(offset, which):
        return pl.multiple_of((2 * ((chip + offset + chips) % WINDOW) + which) * block, block)

    served = [at(-2, 0), at(2, 1)]
    for offset in (1, -1):
        for which in (0, 1):
            served.append(at(offset, which))
    served.append(at(0, 1 - core))
    def everyone(source, target, arrival):
        def chips_away(i, carry):
            away = (chips // 2 - (i + 1) // 2) * (1 - 2 * ((i + 1) % 2))
            for which in (0, 1):
                send(source, target, at(away, which), arrival, arrival)
            return carry

        lax.fori_loop(0, chips - 1, chips_away, 0)
        send(source, target, at(0, 1 - core), arrival, arrival)

    def left(buffer, index):
        pltpu.make_async_remote_copy(
            src_ref=buffer,
            dst_ref=buffer,
            send_sem=send_sem.at[index],
            recv_sem=recv_sem.at[0],
            device_id={"row": at(0, 1 - core)},
            device_id_type=pl.DeviceIdType.MESH,
        ).wait_send()

    sharers = [at(WINDOW * i, core) for i in (2, 1, 3)]

    def send(source, target, device, index, arrival):
        copy = pltpu.make_async_remote_copy(
            src_ref=source,
            dst_ref=target,
            send_sem=send_sem.at[index],
            recv_sem=recv_sem.at[arrival],
            device_id={"row": device},
            device_id_type=pl.DeviceIdType.MESH,
        )
        copy.start()
        return copy

    def arrived(buffer, arrival):
        pltpu.make_async_remote_copy(
            src_ref=buffer,
            dst_ref=buffer,
            send_sem=send_sem.at[0],
            recv_sem=recv_sem.at[arrival],
            device_id={"row": at(0, 1 - core)},
            device_id_type=pl.DeviceIdType.MESH,
        ).wait_recv()

    def load(source, target, index):
        copy = pltpu.make_async_copy(source, target, load_sem.at[index])
        copy.start()
        return copy

    barrier = pltpu.get_barrier_semaphore()

    def greet(i, carry):
        away = (devices // 2 - (i + 1) // 2) * (1 - 2 * ((i + 1) % 2))
        pl.semaphore_signal(
            barrier,
            inc=1,
            device_id={"row": (me + away + devices) % devices},
            device_id_type=pl.DeviceIdType.MESH,
        )
        return carry

    lax.fori_loop(0, devices - 1, greet, 0)

    share = pl.ds(pl.multiple_of(quarter * piece, piece), piece)
    load_targets = load(targets_hbm, targets.at[share], 0)

    def load_a(i, carry):
        place, part = i // quarters, i % quarters
        source = pl.multiple_of((part * 2 * WINDOW + place) * piece, piece)
        target = pl.multiple_of(i * piece, piece)
        pltpu.make_async_copy(
            a_hbm.at[pl.ds(source, piece)], a.at[pl.ds(target, piece)], load_sem.at[1]
        ).start()
        return carry

    lax.fori_loop(0, 2 * WINDOW * quarters, load_a, 0)
    loads = [
        load(diagonal_hbm, diagonal, 2),
        load(lower_hbm, code.at[0], 3),
        load(upper_hbm, code.at[1], 4),
        load(linear_hbm, linear, 5),
    ]

    shown = pl.ds(pl.multiple_of(own + quarter * piece, piece), piece)
    load_targets.wait()
    m[shown, :] = (0.0 - targets[share, :]).astype(BF16)
    pl.semaphore_wait(barrier, devices - 1)
    everyone(m.at[shown], m.at[shown], 3)
    for device in sharers:
        send(targets.at[share], targets.at[share], device, 0, 0)

    pltpu.make_async_copy(a_hbm, a, load_sem.at[1]).wait()
    for copy in loads:
        copy.wait()

    def prepare(i, carry):
        part = pl.ds(pl.multiple_of(i * 128, 128), 128)
        a_t[part, :] = jnp.transpose(a[:, part])
        d = jnp.transpose(jnp.broadcast_to(diagonal[pl.ds(i, 1), :], (128, 128)))
        dd[part, :] = d
        ss[part, :] = 1.0 / (rho_plus_lip + d)
        low[part, :] = code[0, part, :].astype(F32) * (1.0 / 64.0)
        high[part, :] = code[1, part, :].astype(F32) * (1.0 / 64.0)
        return carry

    lax.fori_loop(0, n // 128, prepare, 0)

    arrived(m.at[pl.ds(0, rows - piece)], 3)
    left(m.at[pl.ds(0, rows - piece)], 3)

    gas = [ga_1, ga_2, ga_3]
    gram = []
    first = None
    for it in range(ITERS):
        mine = pl.ds(own, block)
        if it > 0:
            def multiplied(i, carry):
                offset = jnp.where(i == 0, toward, jnp.where(i == 3, 0, 3 - 2 * i))
                part = pl.ds(pl.multiple_of(owned_by(offset, 0), 2 * block), 2 * block)
                product = jnp.dot(a[part, :], xb[...], preferred_element_type=F32)
                pf[part, :] = product
                if it == 1:
                    rounded = product.astype(SENT_A)
                    known_a[part, :] = rounded.astype(F32)
                else:
                    known = known_a[part, :]
                    rounded = (product - known).astype(SENT_A)
                    known_a[part, :] = known + rounded.astype(F32)
                pb[part, :] = rounded

                @pl.when(i < WINDOW - 1)
                def _():
                    for which in (0, 1):
                        send(
                            pb.at[pl.ds(owned_by(offset, which), block)],
                            ra.at[2 * ((i + 2) % 3) + 1 + core],
                            at(offset, which),
                            1,
                            1,
                        )

                return carry

            def based(i, carry):
                part = pl.ds(pl.multiple_of(i * CHUNK, CHUNK), CHUNK)
                z0, u0 = (mz[0, part, :], mu[0, part, :]) if it == 1 else (sz[part, :], su[part, :])
                point = z0 - u0
                base[part, :] = z0 - ss[part, :] * (dd[part, :] * point + linear[part, :])
                return carry

            lax.fori_loop(0, WINDOW, multiplied, 0)
            send(pb.at[pl.ds(owned_by(0, 1 - core), block)], ra.at[0], at(0, 1 - core), 1, 1)
            arrived(ra, 1)
            total = ra[0].astype(F32)
            for i in range(1, len(served)):
                total = total + ra[i].astype(F32)
            if it > 1:
                total = total + window[...]
            window[...] = total
            total = total + pf[mine, :]
            if it > 1:
                total = total - known_b[0]
            rounded = total.astype(SENT_B)
            wb[quarter] = rounded
            known_b[0] = rounded.astype(F32) + (known_b[0] if it > 1 else 0.0)
            send(wb.at[quarter], wb.at[quarter], sharers[0], 2, 2)
            lax.fori_loop(0, n // CHUNK, based, 0)
            for device in sharers[1:]:
                send(wb.at[quarter], wb.at[quarter], device, 2, 2)
            left(ra, 1)
            arrived(wb.at[pl.ds(0, quarters - 1)], 2)
            total = wb[0].astype(F32)
            for i in range(1, quarters):
                total = total + wb[i].astype(F32)
            if it > 1:
                total = total + known_b[1]
            known_b[1] = total
            if it == 1:
                arrived(targets.at[pl.ds(0, (quarters - 1) * piece)], 0)
                left(targets.at[pl.ds(0, (quarters - 1) * piece)], 0)
            m[mine, :] = (total - targets[...]).astype(BF16)
            for device in served:
                send(m.at[mine], m.at[mine], device, 3, 3)
            left(wb.at[pl.ds(0, quarters - 1)], 2)
            arrived(m.at[pl.ds(0, rows - block)], 3)

        def mapped(i, sums):
            part = pl.ds(pl.multiple_of(i * CHUNK, CHUNK), CHUNK)
            gradient = jnp.dot(a_t[part, :], m[...], preferred_element_type=F32)
            if it == 0:
                value = -ss[part, :] * (gradient + linear[part, :])
                z = jnp.minimum(jnp.maximum(value, low[part, :]), high[part, :])
                u = value - z
                mz[0, part, :] = z
                mu[0, part, :] = u
                xb[part, :] = (z - u).astype(BF16)
                return (sums[0] + folded(z * z + u * u),)
            z0, u0 = (mz[0, part, :], mu[0, part, :]) if it == 1 else (sz[part, :], su[part, :])
            value = base[part, :] - ss[part, :] * gradient
            past = [(z0, u0) if it == 1 else (mz[0, part, :], mu[0, part, :])]
            past += [(cz[j, part, :], cu[j, part, :]) for j in range(it - 1)]
            z = jnp.minimum(jnp.maximum(value, low[part, :]), high[part, :])
            u = value - z
            mz[it, part, :] = z
            mu[it, part, :] = u
            dz, du = z - z0, u - u0
            if it < ITERS - 1:
                cz[it - 1, part, :] = dz
                cu[it - 1, part, :] = du
            out = [sums[j] + folded(pz * dz + pu * du) for j, (pz, pu) in enumerate(past)]
            out.append(sums[it] + folded(dz * dz + du * du))
            return tuple(out)

        zero = jnp.zeros((8, s), F32)
        sums = lax.fori_loop(0, n // CHUNK, mapped, (zero,) * (it + 1))
        if it > 0:
            left(m.at[pl.ds(0, rows - block)], 3)
        sums = [jnp.sum(item, axis=0, keepdims=True) for item in sums]
        if it == 0:
            first = sums[0]
            continue
        shared = ([first] if it == 1 else []) + sums
        ga = gas[it - 1]
        for i in range(len(shared)):
            ga[me, pl.ds(i, 1), :] = shared[i]
        everyone(ga.at[me], ga.at[me], 4)
        arrived(ga.at[pl.ds(0, devices - 1)], 4)
        total = jnp.sum(ga[...], axis=0)
        lines = [total[i : i + 1, :] for i in range(len(shared))]
        if it == 1:
            gram = [[lines[0]]]
            lines = lines[1:]
        for i in range(it):
            gram[i].append(lines[i])
        gram.append(lines)
        alpha = mix_weights(gram)

        def combined(i, carry):
            part = pl.ds(pl.multiple_of(i * CHUNK, CHUNK), CHUNK)
            z = alpha[0] * mz[0, part, :]
            u = alpha[0] * mu[0, part, :]
            for j in range(1, it + 1):
                z = z + alpha[j] * mz[j, part, :]
                u = u + alpha[j] * mu[j, part, :]
            z = jnp.minimum(jnp.maximum(z, low[part, :]), high[part, :])
            sz[part, :] = z
            su[part, :] = u
            xb[part, :] = (z - u).astype(BF16)
            return carry

        if it == ITERS - 1:
            for j in range(it + 1):
                last[j][...] = alpha[j]
            left(ga.at[pl.ds(0, devices - 1)], 4)
            break
        lax.fori_loop(0, n // CHUNK, combined, 0)
        left(ga.at[pl.ds(0, devices - 1)], 4)


def per_device(devices, design_matrix, targets, linear, diagonal, lower_code, upper_code):
    rows, n = design_matrix.shape
    s = linear.shape[1]
    quarters = devices // 2 // WINDOW
    block = rows // (2 * WINDOW)
    others = 2 * WINDOW - 1
    full = pltpu.VMEM((n, s), F32)
    hbm = pl.BlockSpec(memory_space=pl.ANY)
    mz, mu, low, high, *alpha = pl.pallas_call(
        functools.partial(kernel, devices),
        out_shape=(
            pltpu.VMEM((ITERS, n, s), F32),
            pltpu.VMEM((ITERS, n, s), F32),
            pltpu.VMEM((n, s), F32),
            pltpu.VMEM((n, s), F32),
            *[pltpu.VMEM((1, s), F32)] * ITERS,
        ),
        in_specs=[hbm] * 6,
        out_specs=(pl.BlockSpec(memory_space=pltpu.VMEM),) * (4 + ITERS),
        scratch_shapes=[
            pltpu.VMEM((rows, n), BF16),
            pltpu.VMEM((n, rows), BF16),
            full,
            pltpu.VMEM((n // 128, 128), F32),
            pltpu.VMEM((2, n, s), jnp.int32),
            full,
            full,
            pltpu.VMEM((ITERS - 2, n, s), F32),
            pltpu.VMEM((ITERS - 2, n, s), F32),
            full,
            full,
            full,
            pltpu.VMEM((n, s), BF16),
            pltpu.VMEM((rows, s), F32),
            pltpu.VMEM((rows, s), SENT_A),
            pltpu.VMEM((rows, s), F32),
            pltpu.VMEM((others, block, s), SENT_A),
            pltpu.VMEM((quarters, block, s), SENT_B),
            pltpu.VMEM((2, block, s), F32),
            pltpu.VMEM((block, s), F32),
            pltpu.VMEM((rows, s), BF16),
            pltpu.VMEM((block, s), F32),
            pltpu.VMEM((devices, 3, s), F32),
            pltpu.VMEM((devices, 3, s), F32),
            pltpu.VMEM((devices, 4, s), F32),
            pltpu.SemaphoreType.DMA((6,)),
            pltpu.SemaphoreType.DMA((5,)),
            pltpu.SemaphoreType.DMA((5,)),
        ],
        compiler_params=pltpu.CompilerParams(
            collective_id=0, has_side_effects=True, vmem_limit_bytes=53 * 1024 * 1024
        ),
        name="admm",
    )(
        design_matrix,
        targets,
        linear,
        diagonal.reshape(n // 128, 128),
        lower_code,
        upper_code,
    )
    z, u = alpha[0] * mz[0], alpha[0] * mu[0]
    for j in range(1, ITERS):
        z, u = z + alpha[j] * mz[j], u + alpha[j] * mu[j]
    return jnp.minimum(jnp.maximum(z, low), high), u


def solution(mesh):
    in_specs = (
        P("groups", "row"),
        P(("groups", "row"), None),
        P(("groups", "row"), None),
        P(("groups", "row")),
        P(("groups", "row"), None),
        P(("groups", "row"), None),
    )
    out_specs = (P(("groups", "row"), None), P(("groups", "row"), None))
    return jax.shard_map(
        functools.partial(per_device, mesh.shape["row"]),
        mesh=mesh,
        in_specs=in_specs,
        out_specs=out_specs,
        check_vma=False,
    )
```
